512 devices in a mesh: groups: 2 (over y), users: 16 (over z), routers: 8 (over x), heads: 2 (over core).
Axes of the slice: x: 8, y: 2, z: 16, core: 2. Of those that a mesh axis runs over, the one named last changes fastest.
The devices are a block of a 8x8x16 slice.
Arguments:
- items: bfloat16 [4096, 64, 1024], P(('groups', 'users', 'routers')), parts along dimension 0, may hold values from -6 to 6
- block_owner: int32 [4096, 1], P(('groups', 'users', 'routers')), parts along dimension 0, may hold values from 0 to 15; in each aligned block of 16 rows (0 to 15, 16 to 31, ...) at most 2 rows name the same one
- block_user: int32 [4096], P(('groups', 'users', 'routers')), parts along dimension 0, may hold values from 0 to 1
- block_fill: int32 [4096], P(('groups', 'users', 'routers')), parts along dimension 0, may hold values from 1 to 64
- prefix_keys: bfloat16 [64, 256, 1024], P(('groups', 'users'), None, 'heads'), parts along dimension 0, may hold values from -6 to 6
- prefix_values: bfloat16 [64, 256, 1024], P(('groups', 'users'), None, 'heads'), parts along dimension 0, may hold values from -6 to 6
- w_in: bfloat16 [4, 1024, 1024], P(None, 'routers', 'heads'), may hold values from -0.1875 to 0.1875
- attn_gain: bfloat16 [1024], P('heads'), may hold values from 0.25 to 1.75
- w_o: bfloat16 [1024, 1024], P('heads', 'routers'), may hold values from -0.1875 to 0.1875
- mlp_gain: bfloat16 [1024], replicated, may hold values from 0.25 to 1.75
- w_one: bfloat16 [1024, 256], replicated, may hold values from -0.1875 to 0.1875
- w_two: bfloat16 [256], replicated, may hold values from -0.375 to 0.375
Outputs:
- scores: float32 [4096, 64], P(('groups', 'users', 'routers')), parts along dimension 0
The draws below stay inside these ranges and needn't reach their ends.
There are 2 independent parts, one for each index of `groups`. The reference program is written for one: setup_inputs(seed, part) draws one part's arguments, and reference() takes and returns one part's arrays. A program takes and returns all parts, laid end to end along the dimension named above; an argument that names none is the same for every part. Nothing has to cross between parts.
Inputs may be any that keep to these rules, and one draw needn't show every extreme that they name: `block_owner`: within the rows of one device (aligned blocks of 16 blocks), no owner is named by more than 2 rows, and in every draw some owner is named by exactly 2 rows of some device.
All inputs are finite; a program needn't handle non-finite values.
Results may differ from the reference program's by a relative error of at most 0.005.
Values may be sent and summed in bfloat16 or wider, within the bound.
No kernel may reach another device: no remote copies, remote signals or barrier semaphores. Data moves between devices by JAX's collectives and lax.ppermute only.
A program may use at most 64 MiB of HBM per device.

```python
import math
import jax
import jax.numpy as jnp
import numpy as np
from jax import lax

D = 1024
HEADS = 8
HEAD_DIM = 128
HID = 256
BLOCK = 64
CAP = 2
LPRE = 256
USR_DEV = 2
BLK_DEV = 16
HD = 1024
USERS = 32
NBLK = 2048
N_USERS = 16


def touch_ends(drawn, own_key, smallest, largest):
    index_at = [jax.random.randint(jax.random.fold_in(own_key, axis), (), 0, length) for axis, length in enumerate(drawn.shape)]
    widest = drawn.shape.index(max(drawn.shape))
    beside = index_at[:widest] + [(index_at[widest] + 1) % drawn.shape[widest]] + index_at[widest + 1:]
    return drawn.at[tuple(index_at)].set(smallest).at[tuple(beside)].set(largest)


def block_scale(rng, dims, split, least, top_value):
    factor_of = 1.0
    for position, shards_of in split:
        draws = jax.random.uniform(jax.random.fold_in(jax.random.fold_in(rng, 6), position), (shards_of,), jnp.float32, least / len(split), top_value / len(split))
        factor_of = factor_of * jnp.repeat(jnp.exp(draws), dims[position] // shards_of).reshape((-1,) + (1,) * (len(dims) - 1 - position))
    return factor_of


def assign_block(rng, own, number, rows, amount, top, limit, skew):
    ranking = jax.random.permutation(rng, amount)
    crowded, ordinary = portions_of(amount, rows * top, limit, skew, True), portions_of(amount, rows * top, limit, skew, False)
    places = jnp.arange(amount)

    def named(tallies, offset_by):
        used = int((tallies > 0).sum())
        fixed = max(1, used // 4)
        passed = fixed + (places - fixed + offset_by * (used - fixed)) % max(1, amount - fixed)
        return jnp.zeros((amount,), jnp.int32).at[ranking[jnp.where(places < fixed, places, passed)]].set(jnp.asarray(tallies, jnp.int32))

    tallies = jnp.where(number % 4 == 0, named(crowded, number // 4), named(ordinary, number - number // 4 - 1))
    mixed = jax.random.permutation(jax.random.fold_in(own, 3), amount)
    source_of, sink = mixed[0:amount // 2 * 2:2], mixed[1:amount // 2 * 2:2]
    slack = jnp.minimum(tallies[source_of] - 1, limit - tallies[sink]) // 2
    slack = jnp.where((source_of == ranking[0]) | (sink == ranking[0]) | (tallies[sink] == 0), 0, jnp.maximum(slack, 0))
    passed = jax.random.randint(jax.random.fold_in(own, 4), (amount // 2,), 0, 1 << 20) % (slack + 1)
    tallies = tallies.at[source_of].add(-passed).at[sink].add(passed)
    items = jnp.searchsorted(jnp.cumsum(tallies), jnp.arange(rows * top), side="right").astype(jnp.int32)
    listing = items.reshape(top, rows).T
    listing = listing[jax.random.permutation(jax.random.fold_in(own, 1), rows)]
    offset_by = jax.random.randint(jax.random.fold_in(own, 2), (rows, 1), 0, top)
    return jnp.take_along_axis(listing, (jnp.arange(top)[None, :] + offset_by) % top, axis=1)


def portions_of(number_of, total, reach, lean, full):
    portions = [(1 << 20) // math.isqrt(rank ** lean) + 1 for rank in range(1, number_of + 1)]
    largest = reach if full else min(reach, max(-(-total // number_of), total * portions[0] // sum(portions)))
    least = 1 if total - largest >= number_of - 1 else 0
    counts, rest = [largest] + [least] * (number_of - 1), total - largest - least * (number_of - 1)
    while rest > 0:
        movable = [i for i in range(1, number_of) if counts[i] < largest] or [i for i in range(1, number_of) if counts[i] < reach]
        pool, remaining = sum([portions[i] for i in movable]), rest
        for i in movable:
            addition = min(reach - counts[i], max(1, remaining * portions[i] // pool), rest)
            counts[i] = counts[i] + addition
            rest = rest - addition
    return np.array(counts)


def gaussian(rng, dims, scale, most, shards=(), held_as=jnp.bfloat16):
    gain = block_scale(rng, dims, shards, -0.22, 0.18) if shards else 1.0
    values = jax.random.normal(rng, dims, jnp.float32) * scale * gain
    return jnp.minimum(jnp.maximum(values, -most), most).astype(held_as)


def setup_inputs(seed: int = 0, part: int = 0) -> dict:
    seeds = jax.random.split(jax.random.key(seed), 13)
    part_splits = jax.random.split(jax.random.fold_in(seeds[12], part), 13)
    items = gaussian(part_splits[0], (NBLK, BLOCK, D), 1.0, 6.0, ((0, 128),))
    block_owner_keys = jax.random.split(jax.random.fold_in(part_splits[1], 1), NBLK // BLK_DEV)
    block_owner_turns = jax.random.permutation(jax.random.fold_in(part_splits[1], 3), NBLK // BLK_DEV)
    block_owner = jax.vmap(lambda own, number: assign_block(jax.random.fold_in(part_splits[1], 2), own, number, BLK_DEV, N_USERS, 1, CAP, 2))(block_owner_keys, block_owner_turns).reshape((NBLK, 1))
    block_user = touch_ends(jax.random.randint(part_splits[2], (NBLK,), 0, USR_DEV), jax.random.fold_in(part_splits[2], 1), 0, USR_DEV - 1).astype(jnp.int32)
    block_fill = touch_ends(jax.random.randint(part_splits[3], (NBLK,), 1, BLOCK + 1), jax.random.fold_in(part_splits[3], 1), 1, BLOCK).astype(jnp.int32)
    prefix_keys = gaussian(part_splits[4], (USERS, LPRE, HD), 1.0, 6.0, ((0, 16), (2, 2)))
    prefix_values = gaussian(part_splits[5], (USERS, LPRE, HD), 1.0, 6.0, ((0, 16), (2, 2)))
    w_in = gaussian(seeds[6], (4, D, HD), D ** -0.5, 0.1875, ((1, 8), (2, 2)))
    attn_gain = jnp.clip(1.0 + 0.15 * jax.random.normal(seeds[7], (HD,), jnp.float32), 0.25, 1.75).astype(jnp.bfloat16)
    w_o = gaussian(seeds[8], (HD, D), HD ** -0.5, 0.1875, ((0, 2), (1, 8)))
    mlp_gain = jnp.clip(1.0 + 0.15 * jax.random.normal(seeds[9], (D,), jnp.float32), 0.25, 1.75).astype(jnp.bfloat16)
    w_one = gaussian(seeds[10], (D, HID), D ** -0.5, 0.1875)
    w_two = gaussian(seeds[11], (HID,), HID ** -0.5, 0.375)
    return dict(items=items, block_owner=block_owner, block_user=block_user, block_fill=block_fill, prefix_keys=prefix_keys, prefix_values=prefix_values, w_in=w_in, attn_gain=attn_gain, w_o=w_o, mlp_gain=mlp_gain, w_one=w_one, w_two=w_two)


def score_block(block_items, owner_index, user_index, fill_count, prefix_keys, prefix_values, wide_in, attn_gain, w_o, mlp_gain, w_one, w_two):
    score_scale = HEAD_DIM ** (-0.5)
    cache_slot = (owner_index * USR_DEV + user_index).astype(jnp.int32)
    user_keys = lax.dynamic_index_in_dim(prefix_keys, cache_slot, 0, keepdims=False)
    user_values = lax.dynamic_index_in_dim(prefix_values, cache_slot, 0, keepdims=False)
    projected = jax.nn.silu(jnp.einsum('rk,pkc->prc', block_items.astype(jnp.float32), wide_in))
    queries = projected[0].astype(jnp.bfloat16)
    query_heads = queries.astype(jnp.float32).reshape(BLOCK, HEADS, HEAD_DIM)
    key_heads = user_keys.astype(jnp.float32).reshape(LPRE, HEADS, HEAD_DIM)
    value_heads = user_values.astype(jnp.float32).reshape(LPRE, HEADS, HEAD_DIM)
    raw_scores = jnp.einsum('qhd,khd->hqk', query_heads, key_heads) * score_scale
    weights = jax.nn.silu(raw_scores).astype(jnp.bfloat16)
    prefix_part = jnp.einsum('hqk,khd->qhd', weights.astype(jnp.float32), value_heads).astype(jnp.bfloat16)
    self_keys = projected[1].reshape(BLOCK, HEADS, HEAD_DIM)
    self_values = projected[2].reshape(BLOCK, HEADS, HEAD_DIM)
    gates = projected[3]
    own_term = jax.nn.silu(lax.optimization_barrier(jnp.sum(query_heads * self_keys, axis=-1)) * score_scale)[..., None] * self_values
    attended = (prefix_part.astype(jnp.float32) + own_term).reshape(BLOCK, HD)
    row_mean = lax.optimization_barrier(jnp.sum(attended, axis=1)) / HD
    row_var = lax.optimization_barrier(jnp.sum(attended * attended, axis=1)) / HD - row_mean * row_mean
    gated = ((attended - row_mean[:, None]) * lax.rsqrt(row_var + 1e-05)[:, None] * attn_gain.astype(jnp.float32) * gates).astype(jnp.bfloat16)
    residual = block_items.astype(jnp.float32) + jnp.dot(gated, w_o, preferred_element_type=jnp.float32)
    row_scale = lax.rsqrt(lax.optimization_barrier(jnp.sum(residual * residual, axis=1)) / D + 1e-05)
    normed = (residual * row_scale[:, None] * mlp_gain.astype(jnp.float32)).astype(jnp.bfloat16)
    hidden = jax.nn.silu(jnp.dot(normed, w_one, preferred_element_type=jnp.float32)).astype(jnp.bfloat16)
    block_scores = jnp.dot(hidden, w_two, preferred_element_type=jnp.float32)
    is_valid = jnp.arange(BLOCK, dtype=jnp.int32) < fill_count
    return jnp.where(is_valid, block_scores, jnp.zeros_like(block_scores))

def reference(items, block_owner, block_user, block_fill, prefix_keys, prefix_values, w_in, attn_gain, w_o, mlp_gain, w_one, w_two):
    wide_in = w_in.astype(jnp.float32)

    def one_block(packed):
        block_items, owner_index, user_index, fill_count = packed
        return score_block(block_items, owner_index, user_index, fill_count, prefix_keys, prefix_values, wide_in, attn_gain, w_o, mlp_gain, w_one, w_two)
    return lax.map(one_block, (items, block_owner[:, 0], block_user, block_fill))
```

```python
import functools

import jax
import jax.numpy as jnp
from jax import lax
from jax.experimental import pallas as pl
from jax.experimental.pallas import tpu as pltpu
from jax.sharding import PartitionSpec as P

HEAD_DIM = 128
CAP = 2
EPSILON = 1e-05
TILE = 256
CHUNK = 256
ALIGN = 16
USER_CODE = 128


def half_silu(half):
    return half * (1.0 + jnp.tanh(half))


def score_kernel(
    code_ref,
    x_ref,
    kt_own,
    kt_other,
    v_own,
    v_other,
    w_own,
    w_other,
    gain_own,
    gain_other,
    wo_own,
    wo_other,
    mlp_gain_ref,
    w_one_ref,
    w_two_ref,
    out_ref,
    rows_ref,
    query_ref,
    prefix_ref,
    own_ref,
    gate_ref,
    score_ref,
    unit_ref,
    offset_ref,
):
    units, unit_rows, width = x_ref.shape
    half_width = v_own.shape[2]
    scale = HEAD_DIM ** (-0.5)

    def place(user, start):
        def step(unit, position):
            code = code_ref[unit]
            count = code % USER_CODE
            mine = (count > 0) & (code // USER_CODE == user)

            @pl.when(mine)
            def _():
                at = pl.multiple_of(position, ALIGN)
                rows_ref[pl.ds(at, unit_rows), :] = x_ref[unit]
                offset_ref[unit] = position

            padded = (count + ALIGN - 1) // ALIGN * ALIGN
            return position + jnp.where(mine, padded, 0)

        return lax.fori_loop(0, units, step, start)

    boundary = place(0, jnp.int32(0))
    total = place(1, boundary)

    def attend(user, queries, kt_ref, values_ref, low):
        raw = jnp.dot(
            queries, kt_ref[user, low : low + HEAD_DIM, :], preferred_element_type=jnp.float32
        )
        weights = half_silu(raw * (0.5 * scale)).astype(jnp.bfloat16)
        return jnp.dot(
            weights,
            values_ref[user, :, low : low + HEAD_DIM],
            preferred_element_type=jnp.float32,
        ).astype(jnp.bfloat16)

    sides = ((kt_own, v_own, w_own, gain_own, wo_own), (kt_other, v_other, w_other, gain_other, wo_other))

    def tile_step(tile, carry):
        start = pl.multiple_of(tile * TILE, TILE)
        x = rows_ref[pl.ds(start, TILE), :]
        first_user = jnp.where(start < boundary, 0, 1)
        mixed = (start < boundary) & (start + TILE > boundary) & (total > boundary)
        for side, (kt_ref, values_ref, w_ref, _, _) in enumerate(sides):
            for low in range(0, half_width, CHUNK):
                at = side * half_width + low

                def projected(which):
                    weight = w_ref[:, which, :, low : low + CHUNK].reshape(width, CHUNK)
                    return half_silu(jnp.dot(x, weight, preferred_element_type=jnp.float32) * 0.5)

                queries = projected(0).astype(jnp.bfloat16)
                query_ref[:, at : at + CHUNK] = queries
                keys = projected(1)
                values = projected(2)
                gate_ref[:, at : at + CHUNK] = projected(3)
                for inner in range(0, CHUNK, HEAD_DIM):
                    part = slice(inner, inner + HEAD_DIM)
                    place_at = slice(at + inner, at + inner + HEAD_DIM)
                    raw = jnp.sum(
                        queries[:, part].astype(jnp.float32) * keys[:, part], axis=1, keepdims=True
                    )
                    own_ref[:, place_at] = half_silu(raw * (0.5 * scale)) * values[:, part]
                    prefix_ref[:, place_at] = attend(
                        first_user, queries[:, part], kt_ref, values_ref, low + inner
                    )

        @pl.when(mixed)
        def _():
            row = start + lax.broadcasted_iota(jnp.int32, (TILE, HEAD_DIM), 0)
            for side, (kt_ref, values_ref, _, _, _) in enumerate(sides):
                for low in range(0, half_width, HEAD_DIM):
                    place_at = slice(side * half_width + low, side * half_width + low + HEAD_DIM)
                    second = attend(1, query_ref[:, place_at], kt_ref, values_ref, low)
                    prefix_ref[:, place_at] = jnp.where(
                        row < boundary, prefix_ref[:, place_at].astype(jnp.float32), second.astype(jnp.float32)
                    ).astype(jnp.bfloat16)

        attended = prefix_ref[...].astype(jnp.float32) + own_ref[...]
        row_mean = jnp.sum(attended, axis=1, keepdims=True) / width
        row_var = jnp.sum(attended * attended, axis=1, keepdims=True) / width - row_mean * row_mean
        inverse = lax.rsqrt(row_var + EPSILON)
        residual = x.astype(jnp.float32)
        for side, (_, _, _, gain_ref, wo_ref) in enumerate(sides):
            part = slice(side * half_width, (side + 1) * half_width)
            gated = (
                (attended[:, part] - row_mean)
                * inverse
                * gain_ref[...].astype(jnp.float32)
                * gate_ref[:, part]
            ).astype(jnp.bfloat16)
            residual = residual + jnp.dot(gated, wo_ref[...], preferred_element_type=jnp.float32)
        squares = jnp.sum(residual * residual, axis=1, keepdims=True)
        normed = (
            residual * lax.rsqrt(squares / width + EPSILON) * mlp_gain_ref[...].astype(jnp.float32)
        ).astype(jnp.bfloat16)
        inner_sum = jnp.dot(normed, w_one_ref[...], preferred_element_type=jnp.float32)
        hidden = half_silu(inner_sum * 0.5).astype(jnp.bfloat16).astype(jnp.float32)
        scores = jnp.sum(hidden * w_two_ref[...].astype(jnp.float32), axis=1, keepdims=True)
        score_ref[pl.ds(start, TILE), :] = jnp.broadcast_to(scores, (TILE, score_ref.shape[1]))
        return carry

    lax.fori_loop(0, (total + TILE - 1) // TILE, tile_step, 0)

    lanes = score_ref.shape[1]
    unit_row = lax.broadcasted_iota(jnp.int32, (unit_rows, lanes), 0)

    def unplace(unit, carry):
        count = code_ref[unit] % USER_CODE
        to = pl.multiple_of(unit * unit_rows, unit_rows)

        @pl.when(count > 0)
        def _():
            at = pl.multiple_of(offset_ref[unit], ALIGN)
            found = score_ref[pl.ds(at, unit_rows), :]
            unit_ref[pl.ds(to, unit_rows), :] = jnp.where(unit_row < count, found, 0.0)

        @pl.when(count == 0)
        def _():
            unit_ref[pl.ds(to, unit_rows), :] = jnp.zeros((unit_rows, lanes), jnp.float32)

        return carry

    lax.fori_loop(0, units, unplace, 0)
    for block in range(units * unit_rows // lanes):
        out_ref[block : block + 1, :] = unit_ref[block * lanes : (block + 1) * lanes, :].T[0:1, :]


def score_units(codes, x, own, other, mlp_gain, w_one, w_two, interpret=False):
    units, unit_rows, width = x.shape
    kt, values, w, gain, wo = own
    kt2, values2, w2, gain2, wo2 = other
    lanes = 128
    rows = units * unit_rows
    room = (rows + TILE - 1) // TILE * TILE + max(TILE, unit_rows)
    vmem = pl.BlockSpec(memory_space=pltpu.VMEM)
    return pl.pallas_call(
        score_kernel,
        out_shape=jax.ShapeDtypeStruct((rows // lanes, lanes), jnp.float32),
        in_specs=[pl.BlockSpec(memory_space=pltpu.SMEM)] + [vmem] * 14,
        out_specs=vmem,
        scratch_shapes=[
            pltpu.VMEM((room, width), jnp.bfloat16),
            pltpu.VMEM((TILE, width), jnp.bfloat16),
            pltpu.VMEM((TILE, width), jnp.bfloat16),
            pltpu.VMEM((TILE, width), jnp.float32),
            pltpu.VMEM((TILE, width), jnp.float32),
            pltpu.VMEM((room, lanes), jnp.float32),
            pltpu.VMEM((rows, lanes), jnp.float32),
            pltpu.SMEM((units,), jnp.int32),
        ],
        compiler_params=pltpu.CompilerParams(vmem_limit_bytes=56 * 1024 * 1024),
        name="score_units",
        interpret=interpret,
    )(
        codes, x, kt, kt2, values, values2, w, w2, gain, gain2, wo, wo2, mlp_gain, w_one, w_two
    )


INTERPRET = False


def local(
    items,
    block_owner,
    block_user,
    block_fill,
    prefix_keys,
    prefix_values,
    w_in,
    attn_gain,
    w_o,
    mlp_gain,
    w_one,
    w_two,
):
    blocks, block_width, model_width = items.shape
    peers = lax.axis_size("users")
    cores = lax.axis_size("heads")
    core = lax.axis_index("heads")
    slots = peers * CAP
    unit_rows = block_width // cores
    flat_items = items.reshape(blocks * block_width, model_width)

    def swapped(x):
        return lax.ppermute(x, "heads", [(k, cores - 1 - k) for k in range(cores)])

    target = block_owner[:, 0]
    earlier = lax.broadcasted_iota(jnp.int32, (blocks, blocks), 1) < lax.broadcasted_iota(
        jnp.int32, (blocks, blocks), 0
    )
    same_target = target[:, None] == target[None, :]
    position = target * CAP + jnp.sum((same_target & earlier).astype(jnp.int32), axis=1)
    selector = lax.broadcasted_iota(jnp.int32, (slots, blocks), 0) == position[None, :]
    code = block_user * USER_CODE + (block_fill + (cores - 1 - core)) // cores
    codes = jnp.sum(jnp.where(selector, code[None, :], 0), axis=1).reshape(peers, CAP)

    inside = lax.broadcasted_iota(jnp.int32, (blocks, block_width), 1)
    goes_to = jnp.where(
        inside % cores == core, position[:, None] * unit_rows + inside // cores, -1
    ).reshape(1, blocks * block_width)
    pick = lax.broadcasted_iota(jnp.int32, (slots * unit_rows, 1), 0) == goes_to
    outgoing = jnp.dot(
        pick.astype(jnp.bfloat16), flat_items, preferred_element_type=jnp.float32
    ).astype(jnp.bfloat16)
    outgoing = outgoing.reshape(peers, CAP * unit_rows, model_width)

    arrived = lax.all_to_all(outgoing, "users", split_axis=0, concat_axis=0, tiled=True)
    arrived_codes = lax.all_to_all(codes, "users", split_axis=0, concat_axis=0, tiled=True)

    w_all = lax.all_gather(w_in, "routers", axis=0)
    wo_all = lax.all_gather(w_o, "routers", axis=1, tiled=True)
    own = (
        jnp.swapaxes(prefix_keys, 1, 2),
        prefix_values,
        w_all,
        attn_gain[None, :],
        wo_all,
    )
    other = jax.tree.map(swapped, own)
    scores = score_units(
        arrived_codes.reshape(slots),
        arrived.reshape(slots, unit_rows, model_width),
        own,
        other,
        mlp_gain[None, :],
        w_one,
        w_two[None, :],
        interpret=INTERPRET,
    )
    scores = scores.reshape(peers, 1, CAP * unit_rows)
    back = jnp.broadcast_to(scores, (peers, cores, CAP * unit_rows)).reshape(peers * cores, -1)
    returned = lax.all_to_all(back, ("users", "heads"), split_axis=0, concat_axis=0, tiled=True)
    returned = returned.reshape(peers, cores, CAP, unit_rows).transpose(0, 2, 3, 1)
    returned = returned.reshape(slots, block_width)
    block_scores = jnp.sum(jnp.where(selector[:, :, None], returned[:, None, :], 0.0), axis=0)
    is_valid = lax.broadcasted_iota(jnp.int32, (blocks, block_width), 1) < block_fill[:, None]
    return jnp.where(is_valid, block_scores, jnp.zeros_like(block_scores))


def solution(mesh):
    placed = (
        P(("groups", "users", "routers"), None, None),
        P(("groups", "users", "routers"), None),
        P(("groups", "users", "routers")),
        P(("groups", "users", "routers")),
        P(("groups", "users"), None, "heads"),
        P(("groups", "users"), None, "heads"),
        P(None, "routers", "heads"),
        P("heads"),
        P("heads", "routers"),
        P(),
        P(),
        P(),
    )
    return jax.shard_map(
        local,
        mesh=mesh,
        in_specs=placed,
        out_specs=P(("groups", "users", "routers"), None),
        check_vma=False,
    )
```

```python
import functools

import jax
import jax.numpy as jnp
from jax import lax
from jax.experimental import pallas as pl
from jax.experimental.pallas import tpu as pltpu
from jax.sharding import PartitionSpec as P

HEAD_DIM = 128
EPSILON = 1e-05
TILE = 256
CHUNK = 256
ALIGN = 16
CODE = 256


def half_silu(half):
    return half * (1.0 + jnp.tanh(half))


def score_kernel(
    base,
    code_ref,
    core_ref,
    x_ref,
    kt_own,
    kt_other,
    v_own,
    v_other,
    gain_own,
    gain_other,
    w_ref,
    mlp_gain_ref,
    w_one_ref,
    w_two_ref,
    out_ref,
    rows_ref,
    prefix_ref,
    own_ref,
    gate_ref,
    wo_ref,
    user_ref,
    score_ref,
    unit_ref,
    offset_ref,
):
    units, unit_rows, width = x_ref.shape
    routers, cores, _, share, _ = w_ref.shape
    half_width = v_own.shape[2]
    scale = HEAD_DIM ** (-0.5)
    core = core_ref[0]
    lanes = score_ref.shape[1]
    unit_row = lax.broadcasted_iota(jnp.int32, (unit_rows, lanes), 0)

    def rows_here(count):
        return jnp.clip((count + (cores - 1 - core)) // cores - base, 0, unit_rows)

    def place(unit, position):
        code = code_ref[unit]
        count = rows_here(code % CODE)
        first = rows_here(code // CODE)

        @pl.when(count > 0)
        def _():
            at = pl.multiple_of(position, ALIGN)
            rows_ref[pl.ds(at, unit_rows), :] = x_ref[unit]
            user_ref[pl.ds(at, unit_rows), :] = (unit_row >= first).astype(jnp.int32)

        offset_ref[unit] = position
        return position + (count + ALIGN - 1) // ALIGN * ALIGN

    total = lax.fori_loop(0, units, place, jnp.int32(0))

    sides = ((kt_own, v_own, gain_own, core), (kt_other, v_other, gain_other, cores - 1 - core))
    for side, (_, _, _, index) in enumerate(sides):
        for router in range(routers):
            for row in range(0, half_width, share):
                wo_ref[
                    side * half_width + row : side * half_width + row + share,
                    router * share : (router + 1) * share,
                ] = w_ref[router, index, row // share, :, half_width : half_width + share]

    def attend(user, queries, kt_ref, values_ref, low):
        raw = jnp.dot(
            queries, kt_ref[user, low : low + HEAD_DIM, :], preferred_element_type=jnp.float32
        )
        weights = half_silu(raw * (0.5 * scale)).astype(jnp.bfloat16)
        return jnp.dot(
            weights,
            values_ref[user, :, low : low + HEAD_DIM],
            preferred_element_type=jnp.float32,
        )

    def tile_step(tile, carry):
        start = pl.multiple_of(tile * TILE, TILE)
        x = rows_ref[pl.ds(start, TILE), :]
        second = user_ref[pl.ds(start, TILE), :] > 0
        for side, (kt_ref, values_ref, _, index) in enumerate(sides):
            for low in range(0, half_width, CHUNK):
                at = side * half_width + low

                def projected(which):
                    weight = w_ref[:, index, which, :, low : low + CHUNK].reshape(width, CHUNK)
                    return half_silu(jnp.dot(x, weight, preferred_element_type=jnp.float32) * 0.5)

                queries = projected(0).astype(jnp.bfloat16)
                keys = projected(1)
                values = projected(2)
                gate_ref[:, at : at + CHUNK] = projected(3)
                for inner in range(0, CHUNK, HEAD_DIM):
                    part = slice(inner, inner + HEAD_DIM)
                    place_at = slice(at + inner, at + inner + HEAD_DIM)
                    raw = jnp.sum(
                        queries[:, part].astype(jnp.float32) * keys[:, part], axis=1, keepdims=True
                    )
                    own_ref[:, place_at] = half_silu(raw * (0.5 * scale)) * values[:, part]
                    prefix_ref[:, place_at] = jnp.where(
                        second,
                        attend(1, queries[:, part], kt_ref, values_ref, low + inner),
                        attend(0, queries[:, part], kt_ref, values_ref, low + inner),
                    ).astype(jnp.bfloat16)

        attended = prefix_ref[...].astype(jnp.float32) + own_ref[...]
        row_mean = jnp.sum(attended, axis=1, keepdims=True) / width
        row_var = jnp.sum(attended * attended, axis=1, keepdims=True) / width - row_mean * row_mean
        inverse = lax.rsqrt(row_var + EPSILON)
        residual = x.astype(jnp.float32)
        for side, (_, _, gain_ref, _) in enumerate(sides):
            part = slice(side * half_width, (side + 1) * half_width)
            gated = (
                (attended[:, part] - row_mean)
                * inverse
                * gain_ref[...].astype(jnp.float32)
                * gate_ref[:, part]
            ).astype(jnp.bfloat16)
            residual = residual + jnp.dot(
                gated, wo_ref[part, :], preferred_element_type=jnp.float32
            )
        squares = jnp.sum(residual * residual, axis=1, keepdims=True)
        normed = (
            residual * lax.rsqrt(squares / width + EPSILON) * mlp_gain_ref[...].astype(jnp.float32)
        ).astype(jnp.bfloat16)
        inner_sum = jnp.dot(normed, w_one_ref[...], preferred_element_type=jnp.float32)
        hidden = half_silu(inner_sum * 0.5).astype(jnp.bfloat16).astype(jnp.float32)
        scores = jnp.sum(hidden * w_two_ref[...].astype(jnp.float32), axis=1, keepdims=True)
        score_ref[pl.ds(start, TILE), :] = jnp.broadcast_to(scores, (TILE, lanes))
        return carry

    lax.fori_loop(0, (total + TILE - 1) // TILE, tile_step, 0)

    def unplace(unit, carry):
        count = rows_here(code_ref[unit] % CODE)
        to = pl.multiple_of(unit * unit_rows, unit_rows)

        @pl.when(count > 0)
        def _():
            at = pl.multiple_of(offset_ref[unit], ALIGN)
            found = score_ref[pl.ds(at, unit_rows), :]
            unit_ref[pl.ds(to, unit_rows), :] = jnp.where(unit_row < count, found, 0.0)

        @pl.when(count == 0)
        def _():
            unit_ref[pl.ds(to, unit_rows), :] = jnp.zeros((unit_rows, lanes), jnp.float32)

        return carry

    lax.fori_loop(0, units, unplace, 0)
    for block in range(units * unit_rows // lanes):
        out_ref[block : block + 1, :] = unit_ref[block * lanes : (block + 1) * lanes, :].T[0:1, :]


def score_units(base, codes, core, x, own, other, w_all, mlp_gain, w_one, w_two):
    units, unit_rows, width = x.shape
    kt, values, gain = own
    kt2, values2, gain2 = other
    lanes = 128
    rows = units * unit_rows
    room = (rows + TILE - 1) // TILE * TILE + max(TILE, unit_rows)
    smem = pl.BlockSpec(memory_space=pltpu.SMEM)
    vmem = pl.BlockSpec(memory_space=pltpu.VMEM)
    return pl.pallas_call(
        functools.partial(score_kernel, base),
        out_shape=jax.ShapeDtypeStruct((rows // lanes, lanes), jnp.float32),
        in_specs=[smem] * 2 + [vmem] * 11,
        out_specs=vmem,
        scratch_shapes=[
            pltpu.VMEM((room, width), jnp.bfloat16),
            pltpu.VMEM((TILE, width), jnp.bfloat16),
            pltpu.VMEM((TILE, width), jnp.float32),
            pltpu.VMEM((TILE, width), jnp.float32),
            pltpu.VMEM((2 * values.shape[2], width), jnp.bfloat16),
            pltpu.VMEM((room, lanes), jnp.int32),
            pltpu.VMEM((room, lanes), jnp.float32),
            pltpu.VMEM((rows, lanes), jnp.float32),
            pltpu.SMEM((units,), jnp.int32),
        ],
        compiler_params=pltpu.CompilerParams(vmem_limit_bytes=VMEM_LIMIT),
        name="score_units",
        interpret=INTERPRET,
    )(codes, core, x, kt, kt2, values, values2, gain, gain2, w_all, mlp_gain, w_one, w_two)


INTERPRET = False
VMEM_LIMIT = 28 * 1024 * 1024


def local(
    items,
    block_owner,
    block_user,
    block_fill,
    prefix_keys,
    prefix_values,
    w_in,
    attn_gain,
    w_o,
    mlp_gain,
    w_one,
    w_two,
):
    blocks, block_width, model_width = items.shape
    peers = lax.axis_size("users")
    cores = lax.axis_size("heads")
    routers = lax.axis_size("routers")
    core = lax.axis_index("heads")
    unit_rows = block_width // cores
    flat_items = items.reshape(blocks * block_width, model_width)

    def swapped(x):
        return lax.ppermute(x, "heads", [(k, cores - 1 - k) for k in range(cores)])

    matrices, share, half_width = w_in.shape
    w_local = jnp.concatenate([w_in, w_o.reshape(matrices, share, share)], axis=2)
    w_all = lax.all_gather(w_local, ("routers", "heads"), axis=0)
    w_all = w_all.reshape(routers, cores, matrices, share, half_width + share)

    target = block_owner[:, 0]
    index = jnp.arange(blocks, dtype=jnp.int32)
    same = target[:, None] == target[None, :]
    ahead = (block_user[None, :] < block_user[:, None]) | (
        (block_user[None, :] == block_user[:, None]) & (index[None, :] < index[:, None])
    )
    packed_start = jnp.sum(jnp.where(same & ahead, block_fill[None, :], 0), axis=1)
    inside = lax.broadcasted_iota(jnp.int32, (blocks, block_width), 1)
    packed = packed_start[:, None] + inside
    here = (inside < block_fill[:, None]) & (packed % cores == core)
    goes_to = jnp.where(here, target[:, None] * block_width + packed // cores, -1)
    goes_to = goes_to.reshape(1, blocks * block_width)

    def packed_half(base):
        slot = lax.broadcasted_iota(jnp.int32, (peers * unit_rows, 1), 0)
        slot = slot // unit_rows * block_width + slot % unit_rows + base
        sent = jnp.dot(
            (slot == goes_to).astype(jnp.bfloat16), flat_items, preferred_element_type=jnp.float32
        )
        return sent.astype(jnp.bfloat16).reshape(peers, unit_rows, model_width)

    def exchanged(x):
        return lax.all_to_all(x, "users", split_axis=0, concat_axis=0, tiled=True)

    bases = (0, unit_rows)
    arrived = [exchanged(packed_half(base)) for base in bases]

    goes = target[None, :] == lax.broadcasted_iota(jnp.int32, (peers, blocks), 0)
    weight = jnp.where(block_user == 0, CODE + 1, 1) * block_fill
    codes = jnp.sum(jnp.where(goes, weight[None, :], 0), axis=1)
    every = lax.all_gather(codes, "users", axis=0)
    me = lax.axis_index("users")
    mine = lax.broadcasted_iota(jnp.int32, (peers, peers), 1) == me
    codes = jnp.sum(jnp.where(mine, every, 0), axis=1)

    own = (jnp.swapaxes(prefix_keys, 1, 2), prefix_values, attn_gain[None, :])
    other = jax.tree.map(swapped, own)
    core_index = core.astype(jnp.int32).reshape(1)
    scores = [
        score_units(
            base, codes, core_index, x, own, other, w_all, mlp_gain[None, :], w_one, w_two[None, :]
        ).reshape(peers, unit_rows)
        for base, x in zip(bases, arrived)
    ]
    returned = exchanged(jnp.concatenate(scores, axis=1))
    returned = jnp.concatenate([returned, swapped(returned)], axis=1)
    row_scores = jnp.sum(
        jnp.where(goes[:, :, None], returned[:, None, :], 0.0), axis=0
    )
    lane = jnp.where(packed % cores == core, 0, block_width) + packed // cores
    wanted = lane[:, :, None] == lax.broadcasted_iota(
        jnp.int32, (blocks, block_width, cores * block_width), 2
    )
    block_scores = jnp.sum(jnp.where(wanted, row_scores[:, None, :], 0.0), axis=2)
    return jnp.where(inside < block_fill[:, None], block_scores, jnp.zeros_like(block_scores))


def solution(mesh):
    placed = (
        P(("groups", "users", "routers"), None, None),
        P(("groups", "users", "routers"), None),
        P(("groups", "users", "routers")),
        P(("groups", "users", "routers")),
        P(("groups", "users"), None, "heads"),
        P(("groups", "users"), None, "heads"),
        P(None, "routers", "heads"),
        P("heads"),
        P("heads", "routers"),
        P(),
        P(),
        P(),
    )
    return jax.shard_map(
        local,
        mesh=mesh,
        in_specs=placed,
        out_specs=P(("groups", "users", "routers"), None),
        check_vma=False,
    )
```

```python
import jax
import jax.numpy as jnp
from jax import lax
from jax.experimental import pallas as pl
from jax.experimental.pallas import tpu as pltpu
from jax.sharding import PartitionSpec as P

HEAD_DIM = 128
EPSILON = 1e-05
TILE = 256
CHUNK = 256
ALIGN = 16
CODE = 256


def half_silu(half):
    return half * (1.0 + jnp.tanh(half))


def score_kernel(
    code_ref,
    core_ref,
    gain_own,
    gain_other,
    mlp_gain_ref,
    w_two_ref,
    x_hbm,
    kt_own,
    kt_other,
    v_own,
    v_other,
    w_hbm,
    w_one_hbm,
    out_ref,
    x_ref,
    kt_ref,
    values_ref,
    w_ref,
    wo_ref,
    w_one_ref,
    rows_ref,
    prefix_ref,
    own_ref,
    gate_ref,
    user_ref,
    score_ref,
    unit_ref,
    offset_ref,
    row_sem,
    chunk_sem,
    wo_sem,
    one_sem,
):
    units, unit_rows, width = x_hbm.shape
    routers, cores, matrices, share, _ = w_hbm.shape
    half_width = v_own.shape[2]
    per_side = half_width // CHUNK
    chunks = width // CHUNK
    scale = HEAD_DIM ** (-0.5)
    core = core_ref[0]
    lanes = score_ref.shape[1]
    unit_row = lax.broadcasted_iota(jnp.int32, (unit_rows, lanes), 0)
    sides = ((kt_own, v_own, core), (kt_other, v_other, cores - 1 - core))

    row_copy = pltpu.make_async_copy(x_hbm, x_ref, row_sem.at[0])
    row_copy.start()
    chunk_copies = []
    for chunk in range(chunks):
        kt, values, index = sides[chunk // per_side]
        low = chunk % per_side * CHUNK
        copies = (
            pltpu.make_async_copy(
                w_hbm.at[:, index, :, :, low : low + CHUNK], w_ref.at[chunk], chunk_sem.at[chunk, 0]
            ),
            pltpu.make_async_copy(
                kt.at[:, low : low + CHUNK, :], kt_ref.at[chunk], chunk_sem.at[chunk, 1]
            ),
            pltpu.make_async_copy(
                values.at[:, :, low : low + CHUNK], values_ref.at[chunk], chunk_sem.at[chunk, 2]
            ),
        )
        for copy in copies:
            copy.start()
        chunk_copies.append(copies)
    tail_copies = []
    for side, (_, _, index) in enumerate(sides):
        for router in range(routers):
            tail_copies.append(
                pltpu.make_async_copy(
                    w_hbm.at[router, index, :, :, half_width : half_width + share],
                    wo_ref.at[side, :, :, router * share : (router + 1) * share],
                    wo_sem.at[side, router],
                )
            )
    tail_copies.append(pltpu.make_async_copy(w_one_hbm, w_one_ref, one_sem.at[0]))
    for copy in tail_copies:
        copy.start()

    def rows_here(count):
        return (count + (cores - 1 - core)) // cores

    def place(unit, position):
        code = code_ref[unit]
        count = rows_here(code % CODE)
        first = rows_here(code // CODE)

        @pl.when(count > 0)
        def _():
            at = pl.multiple_of(position, ALIGN)
            rows_ref[pl.ds(at, unit_rows), :] = x_ref[unit]
            user_ref[pl.ds(at, unit_rows), :] = (unit_row >= first).astype(jnp.int32)

        offset_ref[unit] = position
        return position + (count + ALIGN - 1) // ALIGN * ALIGN

    row_copy.wait()
    total = lax.fori_loop(0, units, place, jnp.int32(0))

    def attend(user, queries, chunk, inner):
        raw = jnp.dot(
            queries,
            kt_ref[chunk, user, inner : inner + HEAD_DIM, :],
            preferred_element_type=jnp.float32,
        )
        weights = half_silu(raw * (0.5 * scale)).astype(jnp.bfloat16)
        return jnp.dot(
            weights,
            values_ref[chunk, user, :, inner : inner + HEAD_DIM],
            preferred_element_type=jnp.float32,
        )

    def tile_step(tile, wait):
        start = pl.multiple_of(tile * TILE, TILE)
        x = rows_ref[pl.ds(start, TILE), :]
        second = user_ref[pl.ds(start, TILE), :] > 0
        for chunk in range(chunks):
            at = chunk * CHUNK
            if wait:
                for copy in chunk_copies[chunk]:
                    copy.wait()

            def projected(which):
                weight = w_ref[chunk, :, which].reshape(width, CHUNK)
                return half_silu(jnp.dot(x, weight, preferred_element_type=jnp.float32) * 0.5)

            queries = projected(0).astype(jnp.bfloat16)
            keys = projected(1)
            values = projected(2)
            gate_ref[:, at : at + CHUNK] = projected(3)
            for inner in range(0, CHUNK, HEAD_DIM):
                part = slice(inner, inner + HEAD_DIM)
                place_at = slice(at + inner, at + inner + HEAD_DIM)
                raw = jnp.sum(
                    queries[:, part].astype(jnp.float32) * keys[:, part], axis=1, keepdims=True
                )
                own_ref[:, place_at] = half_silu(raw * (0.5 * scale)) * values[:, part]
                prefix_ref[:, place_at] = jnp.where(
                    second,
                    attend(1, queries[:, part], chunk, inner),
                    attend(0, queries[:, part], chunk, inner),
                ).astype(jnp.bfloat16)

        if wait:
            for copy in tail_copies:
                copy.wait()
        attended = prefix_ref[...].astype(jnp.float32) + own_ref[...]
        row_mean = jnp.sum(attended, axis=1, keepdims=True) / width
        row_var = jnp.sum(attended * attended, axis=1, keepdims=True) / width - row_mean * row_mean
        inverse = lax.rsqrt(row_var + EPSILON)
        residual = x.astype(jnp.float32)
        for side, gain_ref in enumerate((gain_own, gain_other)):
            part = slice(side * half_width, (side + 1) * half_width)
            gated = (
                (attended[:, part] - row_mean)
                * inverse
                * gain_ref[...].astype(jnp.float32)
                * gate_ref[:, part]
            ).astype(jnp.bfloat16)
            residual = residual + jnp.dot(
                gated,
                wo_ref[side].reshape(half_width, width),
                preferred_element_type=jnp.float32,
            )
        squares = jnp.sum(residual * residual, axis=1, keepdims=True)
        normed = (
            residual * lax.rsqrt(squares / width + EPSILON) * mlp_gain_ref[...].astype(jnp.float32)
        ).astype(jnp.bfloat16)
        inner_sum = jnp.dot(normed, w_one_ref[...], preferred_element_type=jnp.float32)
        hidden = half_silu(inner_sum * 0.5).astype(jnp.bfloat16).astype(jnp.float32)
        scores = jnp.sum(hidden * w_two_ref[...].astype(jnp.float32), axis=1, keepdims=True)
        score_ref[pl.ds(start, TILE), :] = jnp.broadcast_to(scores, (TILE, lanes))

    def later_tile(tile, carry):
        tile_step(tile, False)
        return carry

    tile_step(0, True)
    lax.fori_loop(1, (total + TILE - 1) // TILE, later_tile, 0)

    def unplace(unit, carry):
        count = rows_here(code_ref[unit] % CODE)
        to = pl.multiple_of(unit * unit_rows, unit_rows)

        @pl.when(count > 0)
        def _():
            at = pl.multiple_of(offset_ref[unit], ALIGN)
            found = score_ref[pl.ds(at, unit_rows), :]
            unit_ref[pl.ds(to, unit_rows), :] = jnp.where(unit_row < count, found, 0.0)

        @pl.when(count == 0)
        def _():
            unit_ref[pl.ds(to, unit_rows), :] = jnp.zeros((unit_rows, lanes), jnp.float32)

        return carry

    lax.fori_loop(0, units, unplace, 0)
    for block in range(units * unit_rows // lanes):
        out_ref[block : block + 1, :] = unit_ref[block * lanes : (block + 1) * lanes, :].T[0:1, :]


INTERPRET = False
VMEM_LIMIT = 40 * 1024 * 1024


def score_units(codes, core, x, own, other, w_all, mlp_gain, w_one, w_two):
    units, unit_rows, width = x.shape
    kt, values, gain = own
    kt2, values2, gain2 = other
    users, prefix, half_width = values.shape
    routers, cores, matrices, share, _ = w_all.shape
    chunks = width // CHUNK
    lanes = 128
    rows = units * unit_rows
    room = (rows + TILE - 1) // TILE * TILE + max(TILE, unit_rows)
    smem = pl.BlockSpec(memory_space=pltpu.SMEM)
    vmem = pl.BlockSpec(memory_space=pltpu.VMEM)
    hbm = pl.BlockSpec(memory_space=pltpu.HBM)
    return pl.pallas_call(
        score_kernel,
        out_shape=jax.ShapeDtypeStruct((rows // lanes, lanes), jnp.float32),
        in_specs=[smem] * 2 + [vmem] * 4 + [hbm] * 7,
        out_specs=vmem,
        scratch_shapes=[
            pltpu.VMEM(x.shape, jnp.bfloat16),
            pltpu.VMEM((chunks, users, CHUNK, prefix), jnp.bfloat16),
            pltpu.VMEM((chunks, users, prefix, CHUNK), jnp.bfloat16),
            pltpu.VMEM((chunks, routers, matrices, share, CHUNK), jnp.bfloat16),
            pltpu.VMEM((cores, matrices, share, width), jnp.bfloat16),
            pltpu.VMEM(w_one.shape, jnp.bfloat16),
            pltpu.VMEM((room, width), jnp.bfloat16),
            pltpu.VMEM((TILE, width), jnp.bfloat16),
            pltpu.VMEM((TILE, width), jnp.float32),
            pltpu.VMEM((TILE, width), jnp.float32),
            pltpu.VMEM((room, lanes), jnp.int32),
            pltpu.VMEM((room, lanes), jnp.float32),
            pltpu.VMEM((rows, lanes), jnp.float32),
            pltpu.SMEM((units,), jnp.int32),
            pltpu.SemaphoreType.DMA((1,)),
            pltpu.SemaphoreType.DMA((chunks, 3)),
            pltpu.SemaphoreType.DMA((cores, routers)),
            pltpu.SemaphoreType.DMA((1,)),
        ],
        compiler_params=pltpu.CompilerParams(vmem_limit_bytes=VMEM_LIMIT),
        name="score_units",
        interpret=INTERPRET,
    )(codes, core, gain, gain2, mlp_gain, w_two, x, kt, kt2, values, values2, w_all, w_one)


def local(
    items,
    block_owner,
    block_user,
    block_fill,
    prefix_keys,
    prefix_values,
    w_in,
    attn_gain,
    w_o,
    mlp_gain,
    w_one,
    w_two,
):
    blocks, block_width, model_width = items.shape
    peers = lax.axis_size("users")
    cores = lax.axis_size("heads")
    routers = lax.axis_size("routers")
    core = lax.axis_index("heads")
    flat_items = items.reshape(blocks * block_width, model_width)

    def swapped(x):
        return lax.ppermute(x, "heads", [(k, cores - 1 - k) for k in range(cores)])

    def exchanged(x):
        return lax.all_to_all(x, "users", split_axis=0, concat_axis=0, tiled=True)

    target = block_owner[:, 0]
    goes = target[None, :] == lax.broadcasted_iota(jnp.int32, (peers, blocks), 0)
    weight = jnp.where(block_user == 0, CODE + 1, 1) * block_fill
    codes = jnp.sum(jnp.where(goes, weight[None, :], 0), axis=1)
    codes = exchanged(codes.reshape(peers, 1)).reshape(peers)

    index = jnp.arange(blocks, dtype=jnp.int32)
    same = target[:, None] == target[None, :]
    ahead = (block_user[None, :] < block_user[:, None]) | (
        (block_user[None, :] == block_user[:, None]) & (index[None, :] < index[:, None])
    )
    packed_start = jnp.sum(jnp.where(same & ahead, block_fill[None, :], 0), axis=1)
    inside = lax.broadcasted_iota(jnp.int32, (blocks, block_width), 1)
    packed = packed_start[:, None] + inside
    here = (inside < block_fill[:, None]) & (packed % cores == core)
    goes_to = jnp.where(here, target[:, None] * block_width + packed // cores, -1)
    goes_to = goes_to.reshape(1, blocks * block_width)
    slot = lax.broadcasted_iota(jnp.int32, (peers * block_width, 1), 0)
    sent = jnp.dot(
        (slot == goes_to).astype(jnp.bfloat16), flat_items, preferred_element_type=jnp.float32
    ).astype(jnp.bfloat16)
    arrived = exchanged(sent.reshape(peers, block_width, model_width))

    matrices, share, half_width = w_in.shape
    w_local = jnp.concatenate([w_in, w_o.reshape(matrices, share, share)], axis=2)
    w_all = lax.all_gather(w_local, ("routers", "heads"), axis=0)
    w_all = w_all.reshape(routers, cores, matrices, share, half_width + share)
    own = (jnp.swapaxes(prefix_keys, 1, 2), prefix_values, attn_gain[None, :])
    other = jax.tree.map(swapped, own)
    core_index = core.astype(jnp.int32).reshape(1)
    scores = score_units(
        codes, core_index, arrived, own, other, w_all, mlp_gain[None, :], w_one, w_two[None, :]
    ).reshape(peers, block_width)
    returned = exchanged(scores)
    returned = jnp.concatenate([returned, swapped(returned)], axis=1)
    row_scores = jnp.sum(jnp.where(goes[:, :, None], returned[:, None, :], 0.0), axis=0)
    lane = jnp.where(packed % cores == core, 0, block_width) + packed // cores
    wanted = lane[:, :, None] == lax.broadcasted_iota(
        jnp.int32, (blocks, block_width, cores * block_width), 2
    )
    block_scores = jnp.sum(jnp.where(wanted, row_scores[:, None, :], 0.0), axis=2)
    return jnp.where(inside < block_fill[:, None], block_scores, jnp.zeros_like(block_scores))


def solution(mesh):
    placed = (
        P(("groups", "users", "routers"), None, None),
        P(("groups", "users", "routers"), None),
        P(("groups", "users", "routers")),
        P(("groups", "users", "routers")),
        P(("groups", "users"), None, "heads"),
        P(("groups", "users"), None, "heads"),
        P(None, "routers", "heads"),
        P("heads"),
        P("heads", "routers"),
        P(),
        P(),
        P(),
    )
    return jax.shard_map(
        local,
        mesh=mesh,
        in_specs=placed,
        out_specs=P(("groups", "users", "routers"), None),
        check_vma=False,
    )
```

```python
import jax
import jax.numpy as jnp
from jax import lax
from jax.experimental import pallas as pl
from jax.experimental.pallas import tpu as pltpu
from jax.sharding import PartitionSpec as P


HEAD_DIM = 128
EPSILON = 1e-05
TILE = 256
CHUNK = 256
ALIGN = 16
CODE = 256


def half_silu(half):
    return half * (1.0 + jnp.tanh(half))


def score_kernel(
    code_ref,
    core_ref,
    gain_own,
    gain_other,
    mlp_gain_ref,
    w_two_ref,
    x_hbm,
    kt_own,
    kt_other,
    v_own,
    v_other,
    w_own,
    w_other,
    w_one_hbm,
    out_ref,
    x_ref,
    kt_ref,
    values_ref,
    w_ref,
    wo_ref,
    w_one_ref,
    rows_ref,
    prefix_ref,
    own_ref,
    gate_ref,
    user_ref,
    score_ref,
    unit_ref,
    offset_ref,
    row_sem,
    chunk_sem,
    wo_sem,
    one_sem,
):
    units, unit_rows, width = x_hbm.shape
    routers, _, share, _ = w_own.shape
    half_width = v_own.shape[2]
    cores = width // half_width
    per_side = half_width // CHUNK
    chunks = width // CHUNK
    scale = HEAD_DIM ** (-0.5)
    core = core_ref[0]
    router_here = core_ref[1]
    lanes = score_ref.shape[1]
    unit_row = lax.broadcasted_iota(jnp.int32, (unit_rows, lanes), 0)
    sides = ((kt_own, v_own, w_own), (kt_other, v_other, w_other))

    def ring_index(router):
        ahead = router - router_here
        return jnp.where(ahead < 0, ahead + routers, ahead)

    row_copy = pltpu.make_async_copy(x_hbm, x_ref, row_sem.at[0])
    row_copy.start()
    chunk_copies = []
    for chunk in range(chunks):
        kt, values, weights = sides[chunk // per_side]
        low = chunk % per_side * CHUNK
        copies = [
            pltpu.make_async_copy(
                weights.at[ring_index(router), :, :, low : low + CHUNK],
                w_ref.at[chunk, router],
                chunk_sem.at[chunk, router],
            )
            for router in range(routers)
        ]
        copies += [
            pltpu.make_async_copy(
                kt.at[:, low : low + CHUNK, :], kt_ref.at[chunk], chunk_sem.at[chunk, routers]
            ),
            pltpu.make_async_copy(
                values.at[:, :, low : low + CHUNK],
                values_ref.at[chunk],
                chunk_sem.at[chunk, routers + 1],
            ),
        ]
        for copy in copies:
            copy.start()
        chunk_copies.append(copies)
    tail_copies = []
    for side, (_, _, weights) in enumerate(sides):
        for router in range(routers):
            tail_copies.append(
                pltpu.make_async_copy(
                    weights.at[ring_index(router), :, :, half_width : half_width + share],
                    wo_ref.at[side, :, :, router * share : (router + 1) * share],
                    wo_sem.at[side, router],
                )
            )
    tail_copies.append(pltpu.make_async_copy(w_one_hbm, w_one_ref, one_sem.at[0]))
    for copy in tail_copies:
        copy.start()

    def rows_here(count):
        return (count + (cores - 1 - core)) // cores

    def place(unit, position):
        code = code_ref[unit]
        count = rows_here(code % CODE)
        first = rows_here(code // CODE)

        @pl.when(count > 0)
        def _():
            at = pl.multiple_of(position, ALIGN)
            rows_ref[pl.ds(at, unit_rows), :] = x_ref[unit]
            user_ref[pl.ds(at, unit_rows), :] = (unit_row >= first).astype(jnp.int32)

        offset_ref[unit] = position
        return position + (count + ALIGN - 1) // ALIGN * ALIGN

    row_copy.wait()
    total = lax.fori_loop(0, units, place, jnp.int32(0))

    def attend(user, queries, chunk, inner):
        raw = jnp.dot(
            queries,
            kt_ref[chunk, user, inner : inner + HEAD_DIM, :],
            preferred_element_type=jnp.float32,
        )
        weights = half_silu(raw * (0.5 * scale)).astype(jnp.bfloat16)
        return jnp.dot(
            weights,
            values_ref[chunk, user, :, inner : inner + HEAD_DIM],
            preferred_element_type=jnp.float32,
        )

    def tile_step(tile, wait):
        start = pl.multiple_of(tile * TILE, TILE)
        x = rows_ref[pl.ds(start, TILE), :]
        second = user_ref[pl.ds(start, TILE), :] > 0
        for chunk in range(chunks):
            at = chunk * CHUNK
            if wait:
                for copy in chunk_copies[chunk]:
                    copy.wait()

            def projected(which):
                weight = w_ref[chunk, :, which].reshape(width, CHUNK)
                return half_silu(jnp.dot(x, weight, preferred_element_type=jnp.float32) * 0.5)

            queries = projected(0).astype(jnp.bfloat16)
            keys = projected(1)
            values = projected(2)
            gate_ref[:, at : at + CHUNK] = projected(3)
            for inner in range(0, CHUNK, HEAD_DIM):
                part = slice(inner, inner + HEAD_DIM)
                place_at = slice(at + inner, at + inner + HEAD_DIM)
                raw = jnp.sum(
                    queries[:, part].astype(jnp.float32) * keys[:, part], axis=1, keepdims=True
                )
                own_ref[:, place_at] = half_silu(raw * (0.5 * scale)) * values[:, part]
                prefix_ref[:, place_at] = jnp.where(
                    second,
                    attend(1, queries[:, part], chunk, inner),
                    attend(0, queries[:, part], chunk, inner),
                ).astype(jnp.bfloat16)

        if wait:
            for copy in tail_copies:
                copy.wait()
        attended = prefix_ref[...].astype(jnp.float32) + own_ref[...]
        row_mean = jnp.sum(attended, axis=1, keepdims=True) / width
        row_var = jnp.sum(attended * attended, axis=1, keepdims=True) / width - row_mean * row_mean
        inverse = lax.rsqrt(row_var + EPSILON)
        residual = x.astype(jnp.float32)
        for side, gain_ref in enumerate((gain_own, gain_other)):
            part = slice(side * half_width, (side + 1) * half_width)
            gated = (
                (attended[:, part] - row_mean)
                * inverse
                * gain_ref[...].astype(jnp.float32)
                * gate_ref[:, part]
            ).astype(jnp.bfloat16)
            residual = residual + jnp.dot(
                gated,
                wo_ref[side].reshape(half_width, width),
                preferred_element_type=jnp.float32,
            )
        squares = jnp.sum(residual * residual, axis=1, keepdims=True)
        normed = (
            residual * lax.rsqrt(squares / width + EPSILON) * mlp_gain_ref[...].astype(jnp.float32)
        ).astype(jnp.bfloat16)
        inner_sum = jnp.dot(normed, w_one_ref[...], preferred_element_type=jnp.float32)
        hidden = half_silu(inner_sum * 0.5).astype(jnp.bfloat16).astype(jnp.float32)
        scores = jnp.sum(hidden * w_two_ref[...].astype(jnp.float32), axis=1, keepdims=True)
        score_ref[pl.ds(start, TILE), :] = jnp.broadcast_to(scores, (TILE, lanes))

    def later_tile(tile, carry):
        tile_step(tile, False)
        return carry

    tile_step(0, True)
    lax.fori_loop(1, (total + TILE - 1) // TILE, later_tile, 0)

    def unplace(unit, carry):
        count = rows_here(code_ref[unit] % CODE)
        to = pl.multiple_of(unit * unit_rows, unit_rows)

        @pl.when(count > 0)
        def _():
            at = pl.multiple_of(offset_ref[unit], ALIGN)
            found = score_ref[pl.ds(at, unit_rows), :]
            unit_ref[pl.ds(to, unit_rows), :] = jnp.where(unit_row < count, found, 0.0)

        @pl.when(count == 0)
        def _():
            unit_ref[pl.ds(to, unit_rows), :] = jnp.zeros((unit_rows, lanes), jnp.float32)

        return carry

    lax.fori_loop(0, units, unplace, 0)
    for block in range(units * unit_rows // lanes):
        out_ref[block : block + 1, :] = unit_ref[block * lanes : (block + 1) * lanes, :].T[0:1, :]


INTERPRET = False
VMEM_LIMIT = 40 * 1024 * 1024


def score_units(codes, core, x, own, other, mlp_gain, w_one, w_two):
    units, unit_rows, width = x.shape
    kt, values, gain, w = own
    kt2, values2, gain2, w2 = other
    users, prefix, half_width = values.shape
    routers, matrices, share, _ = w.shape
    cores = width // half_width
    chunks = width // CHUNK
    lanes = 128
    rows = units * unit_rows
    room = (rows + TILE - 1) // TILE * TILE + max(TILE, unit_rows)
    smem = pl.BlockSpec(memory_space=pltpu.SMEM)
    vmem = pl.BlockSpec(memory_space=pltpu.VMEM)
    hbm = pl.BlockSpec(memory_space=pltpu.HBM)
    return pl.pallas_call(
        score_kernel,
        out_shape=jax.ShapeDtypeStruct((rows // lanes, lanes), jnp.float32),
        in_specs=[smem] * 2 + [vmem] * 4 + [hbm] * 8,
        out_specs=vmem,
        scratch_shapes=[
            pltpu.VMEM(x.shape, jnp.bfloat16),
            pltpu.VMEM((chunks, users, CHUNK, prefix), jnp.bfloat16),
            pltpu.VMEM((chunks, users, prefix, CHUNK), jnp.bfloat16),
            pltpu.VMEM((chunks, routers, matrices, share, CHUNK), jnp.bfloat16),
            pltpu.VMEM((cores, matrices, share, width), jnp.bfloat16),
            pltpu.VMEM(w_one.shape, jnp.bfloat16),
            pltpu.VMEM((room, width), jnp.bfloat16),
            pltpu.VMEM((TILE, width), jnp.bfloat16),
            pltpu.VMEM((TILE, width), jnp.float32),
            pltpu.VMEM((TILE, width), jnp.float32),
            pltpu.VMEM((room, lanes), jnp.int32),
            pltpu.VMEM((room, lanes), jnp.float32),
            pltpu.VMEM((rows, lanes), jnp.float32),
            pltpu.SMEM((units,), jnp.int32),
            pltpu.SemaphoreType.DMA((1,)),
            pltpu.SemaphoreType.DMA((chunks, routers + 2)),
            pltpu.SemaphoreType.DMA((cores, routers)),
            pltpu.SemaphoreType.DMA((1,)),
        ],
        compiler_params=pltpu.CompilerParams(vmem_limit_bytes=VMEM_LIMIT),
        name="score_units",
        interpret=INTERPRET,
    )(codes, core, gain, gain2, mlp_gain, w_two, x, kt, kt2, values, values2, w, w2, w_one)


def local(
    items,
    block_owner,
    block_user,
    block_fill,
    prefix_keys,
    prefix_values,
    w_in,
    attn_gain,
    w_o,
    mlp_gain,
    w_one,
    w_two,
):
    blocks, block_width, model_width = items.shape
    peers = lax.axis_size("users")
    cores = lax.axis_size("heads")
    routers = lax.axis_size("routers")
    core = lax.axis_index("heads")
    flat_items = items.reshape(blocks * block_width, model_width)

    def swapped(x):
        return lax.ppermute(x, "heads", [(k, cores - 1 - k) for k in range(cores)])

    def exchanged(x):
        return lax.all_to_all(x, "users", split_axis=0, concat_axis=0, tiled=True)

    target = block_owner[:, 0]
    me = lax.axis_index("users")

    index = jnp.arange(blocks, dtype=jnp.int32)
    same = target[:, None] == target[None, :]
    ahead = (block_user[None, :] < block_user[:, None]) | (
        (block_user[None, :] == block_user[:, None]) & (index[None, :] < index[:, None])
    )
    packed_start = jnp.sum(jnp.where(same & ahead, block_fill[None, :], 0), axis=1)
    inside = lax.broadcasted_iota(jnp.int32, (blocks, block_width), 1)
    packed = packed_start[:, None] + inside
    here = (inside < block_fill[:, None]) & (packed % cores == core)
    goes_to = jnp.where(here, target[:, None] * block_width + packed // cores, -1)
    goes_to = goes_to.reshape(1, blocks * block_width)
    slot = lax.broadcasted_iota(jnp.int32, (peers * block_width, 1), 0)
    sent = jnp.dot(
        (slot == goes_to).astype(jnp.bfloat16), flat_items, preferred_element_type=jnp.float32
    ).astype(jnp.bfloat16)
    sent, block_user, w_in = lax.optimization_barrier((sent, block_user, w_in))
    arrived = exchanged(sent.reshape(peers, block_width, model_width))

    goes = target[None, :] == lax.broadcasted_iota(jnp.int32, (peers, blocks), 0)
    weight = jnp.where(block_user == 0, CODE + 1, 1) * block_fill
    every = jnp.sum(jnp.where(goes, weight[None, :], 0), axis=1)[None, :]
    while every.shape[0] < peers:
        step = every.shape[0]
        pairs = [(k, (k + step) % peers) for k in range(peers)]
        every = jnp.concatenate([every, lax.ppermute(every, "users", pairs)], axis=0)
    source = (me + peers - lax.broadcasted_iota(jnp.int32, (peers, peers, peers), 1)) % peers
    wanted = (source == lax.broadcasted_iota(jnp.int32, (peers, peers, peers), 0)) & (
        lax.broadcasted_iota(jnp.int32, (peers, peers, peers), 2) == me
    )
    codes = jnp.sum(jnp.where(wanted, every[None], 0), axis=(1, 2))

    matrices, share, _ = w_in.shape
    w_local = jnp.concatenate([w_in, w_o.reshape(matrices, share, share)], axis=2)
    up = [(k, (k + 1) % routers) for k in range(routers)]
    down = [(k, (k - 1) % routers) for k in range(routers)]
    from_below, from_above = w_local, w_local
    ring = {0: w_local}
    for step in range(1, routers // 2):
        from_below = lax.ppermute(from_below, "routers", up)
        from_above = lax.ppermute(from_above, "routers", down)
        ring[routers - step] = from_below
        ring[step] = from_above
    half = matrices // 2
    ring[routers // 2] = jnp.concatenate(
        [
            lax.ppermute(from_below[:half], "routers", up),
            lax.ppermute(from_above[half:], "routers", down),
        ],
        axis=0,
    )
    w_ring = jnp.stack([ring[k] for k in range(routers)])
    own = (jnp.swapaxes(prefix_keys, 1, 2), prefix_values, attn_gain[None, :], w_ring)
    other = jax.tree.map(swapped, own)
    core_index = jnp.stack([core, lax.axis_index("routers")]).astype(jnp.int32)
    scores = score_units(
        codes, core_index, arrived, own, other, mlp_gain[None, :], w_one, w_two[None, :]
    ).reshape(peers, block_width)
    returned = exchanged(scores)
    returned = jnp.concatenate([returned, swapped(returned)], axis=1)
    row_scores = jnp.sum(jnp.where(goes[:, :, None], returned[:, None, :], 0.0), axis=0)
    lane = jnp.where(packed % cores == core, 0, block_width) + packed // cores
    wanted = lane[:, :, None] == lax.broadcasted_iota(
        jnp.int32, (blocks, block_width, cores * block_width), 2
    )
    block_scores = jnp.sum(jnp.where(wanted, row_scores[:, None, :], 0.0), axis=2)
    return jnp.where(inside < block_fill[:, None], block_scores, jnp.zeros_like(block_scores))


def solution(mesh):
    placed = (
        P(("groups", "users", "routers"), None, None),
        P(("groups", "users", "routers"), None),
        P(("groups", "users", "routers")),
        P(("groups", "users", "routers")),
        P(("groups", "users"), None, "heads"),
        P(("groups", "users"), None, "heads"),
        P(None, "routers", "heads"),
        P("heads"),
        P("heads", "routers"),
        P(),
        P(),
        P(),
    )
    return jax.shard_map(
        local,
        mesh=mesh,
        in_specs=placed,
        out_specs=P(("groups", "users", "routers"), None),
        check_vma=False,
    )
```

```python
import jax
import jax.numpy as jnp
from jax import lax
from jax.experimental import pallas as pl
from jax.experimental.pallas import tpu as pltpu
from jax.sharding import PartitionSpec as P


HEAD_DIM = 128
EPSILON = 1e-05
TILE = 256
CHUNK = 256
ALIGN = 16
CODE = 256


def half_silu(half):
    return half * (1.0 + jnp.tanh(half))


def score_kernel(
    code_ref,
    core_ref,
    gain_own,
    gain_other,
    mlp_gain_ref,
    w_two_ref,
    x_hbm,
    kt_own,
    kt_other,
    v_own,
    v_other,
    w_own,
    w_other,
    w_one_hbm,
    out_ref,
    x_ref,
    kt_ref,
    values_ref,
    w_ref,
    wo_ref,
    w_one_ref,
    rows_ref,
    prefix_ref,
    own_ref,
    gate_ref,
    user_ref,
    score_ref,
    unit_ref,
    offset_ref,
    row_sem,
    chunk_sem,
    wo_sem,
    one_sem,
):
    units, unit_rows, width = x_hbm.shape
    routers, _, share, _ = w_own.shape
    half_width = v_own.shape[2]
    cores = width // half_width
    per_side = half_width // CHUNK
    chunks = width // CHUNK
    scale = HEAD_DIM ** (-0.5)
    core = core_ref[0]
    router_here = core_ref[1]
    lanes = score_ref.shape[1]
    unit_row = lax.broadcasted_iota(jnp.int32, (unit_rows, lanes), 0)
    sides = ((kt_own, v_own, w_own), (kt_other, v_other, w_other))

    def ring_index(router):
        ahead = router - router_here
        return jnp.where(ahead < 0, ahead + routers, ahead)

    row_copy = pltpu.make_async_copy(x_hbm, x_ref, row_sem.at[0])
    row_copy.start()
    chunk_copies = []
    for chunk in range(chunks):
        kt, values, weights = sides[chunk // per_side]
        low = chunk % per_side * CHUNK
        copies = [
            pltpu.make_async_copy(
                weights.at[ring_index(router), :, :, low : low + CHUNK],
                w_ref.at[chunk, router],
                chunk_sem.at[chunk, router],
            )
            for router in range(routers)
        ]
        copies += [
            pltpu.make_async_copy(
                kt.at[:, low : low + CHUNK, :], kt_ref.at[chunk], chunk_sem.at[chunk, routers]
            ),
            pltpu.make_async_copy(
                values.at[:, :, low : low + CHUNK],
                values_ref.at[chunk],
                chunk_sem.at[chunk, routers + 1],
            ),
        ]
        for copy in copies:
            copy.start()
        chunk_copies.append(copies)
    tail_copies = []
    for side, (_, _, weights) in enumerate(sides):
        for router in range(routers):
            tail_copies.append(
                pltpu.make_async_copy(
                    weights.at[ring_index(router), :, :, half_width : half_width + share],
                    wo_ref.at[side, :, :, router * share : (router + 1) * share],
                    wo_sem.at[side, router],
                )
            )
    tail_copies.append(pltpu.make_async_copy(w_one_hbm, w_one_ref, one_sem.at[0]))
    for copy in tail_copies:
        copy.start()

    def rows_here(count):
        return (count + (cores - 1 - core)) // cores

    def place(unit, position):
        code = code_ref[unit]
        count = rows_here(code % CODE)
        first = rows_here(code // CODE)

        @pl.when(count > 0)
        def _():
            at = pl.multiple_of(position, ALIGN)
            rows_ref[pl.ds(at, unit_rows), :] = x_ref[unit]
            user_ref[pl.ds(at, unit_rows), :] = (unit_row >= first).astype(jnp.int32)

        offset_ref[unit] = position
        return position + (count + ALIGN - 1) // ALIGN * ALIGN

    row_copy.wait()
    total = lax.fori_loop(0, units, place, jnp.int32(0))

    def attend(user, queries, chunk, inner):
        raw = jnp.dot(
            queries,
            kt_ref[chunk, user, inner : inner + HEAD_DIM, :],
            preferred_element_type=jnp.float32,
        )
        weights = half_silu(raw * (0.5 * scale)).astype(jnp.bfloat16)
        return jnp.dot(
            weights,
            values_ref[chunk, user, :, inner : inner + HEAD_DIM],
            preferred_element_type=jnp.float32,
        )

    def tile_step(tile, wait):
        start = pl.multiple_of(tile * TILE, TILE)
        x = rows_ref[pl.ds(start, TILE), :]
        second = user_ref[pl.ds(start, TILE), :] > 0
        for chunk in range(chunks):
            at = chunk * CHUNK
            if wait:
                for copy in chunk_copies[chunk]:
                    copy.wait()

            def projected(which):
                weight = w_ref[chunk, :, which].reshape(width, CHUNK)
                return half_silu(jnp.dot(x, weight, preferred_element_type=jnp.float32) * 0.5)

            queries = projected(0).astype(jnp.bfloat16)
            keys = projected(1)
            values = projected(2)
            gate_ref[:, at : at + CHUNK] = projected(3)
            for inner in range(0, CHUNK, HEAD_DIM):
                part = slice(inner, inner + HEAD_DIM)
                place_at = slice(at + inner, at + inner + HEAD_DIM)
                raw = jnp.sum(
                    queries[:, part].astype(jnp.float32) * keys[:, part], axis=1, keepdims=True
                )
                own_ref[:, place_at] = half_silu(raw * (0.5 * scale)) * values[:, part]
                prefix_ref[:, place_at] = jnp.where(
                    second,
                    attend(1, queries[:, part], chunk, inner),
                    attend(0, queries[:, part], chunk, inner),
                ).astype(jnp.bfloat16)

        if wait:
            for copy in tail_copies:
                copy.wait()
        attended = prefix_ref[...].astype(jnp.float32) + own_ref[...]
        row_mean = jnp.sum(attended, axis=1, keepdims=True) / width
        row_var = jnp.sum(attended * attended, axis=1, keepdims=True) / width - row_mean * row_mean
        inverse = lax.rsqrt(row_var + EPSILON)
        residual = x.astype(jnp.float32)
        for side, gain_ref in enumerate((gain_own, gain_other)):
            part = slice(side * half_width, (side + 1) * half_width)
            gated = (
                (attended[:, part] - row_mean)
                * inverse
                * gain_ref[...].astype(jnp.float32)
                * gate_ref[:, part]
            ).astype(jnp.bfloat16)
            residual = residual + jnp.dot(
                gated,
                wo_ref[side].reshape(half_width, width),
                preferred_element_type=jnp.float32,
            )
        squares = jnp.sum(residual * residual, axis=1, keepdims=True)
        normed = (
            residual * lax.rsqrt(squares / width + EPSILON) * mlp_gain_ref[...].astype(jnp.float32)
        ).astype(jnp.bfloat16)
        inner_sum = jnp.dot(normed, w_one_ref[...], preferred_element_type=jnp.float32)
        hidden = half_silu(inner_sum * 0.5).astype(jnp.bfloat16).astype(jnp.float32)
        scores = jnp.sum(hidden * w_two_ref[...].astype(jnp.float32), axis=1, keepdims=True)
        score_ref[pl.ds(start, TILE), :] = jnp.broadcast_to(scores, (TILE, lanes))

    def later_tile(tile, carry):
        tile_step(tile, False)
        return carry

    tile_step(0, True)
    lax.fori_loop(1, (total + TILE - 1) // TILE, later_tile, 0)

    def unplace(unit, carry):
        count = rows_here(code_ref[unit] % CODE)
        to = pl.multiple_of(unit * unit_rows, unit_rows)

        @pl.when(count > 0)
        def _():
            at = pl.multiple_of(offset_ref[unit], ALIGN)
            found = score_ref[pl.ds(at, unit_rows), :]
            unit_ref[pl.ds(to, unit_rows), :] = jnp.where(unit_row < count, found, 0.0)

        @pl.when(count == 0)
        def _():
            unit_ref[pl.ds(to, unit_rows), :] = jnp.zeros((unit_rows, lanes), jnp.float32)

        return carry

    lax.fori_loop(0, units, unplace, 0)
    for block in range(units * unit_rows // lanes):
        out_ref[block : block + 1, :] = unit_ref[block * lanes : (block + 1) * lanes, :].T[0:1, :]


INTERPRET = False
VMEM_LIMIT = 40 * 1024 * 1024


def score_units(codes, core, x, own, other, mlp_gain, w_one, w_two):
    units, unit_rows, width = x.shape
    kt, values, gain, w = own
    kt2, values2, gain2, w2 = other
    users, prefix, half_width = values.shape
    routers, matrices, share, _ = w.shape
    cores = width // half_width
    chunks = width // CHUNK
    lanes = 128
    rows = units * unit_rows
    room = (rows + TILE - 1) // TILE * TILE + max(TILE, unit_rows)
    smem = pl.BlockSpec(memory_space=pltpu.SMEM)
    vmem = pl.BlockSpec(memory_space=pltpu.VMEM)
    hbm = pl.BlockSpec(memory_space=pltpu.HBM)
    return pl.pallas_call(
        score_kernel,
        out_shape=jax.ShapeDtypeStruct((rows // lanes, lanes), jnp.float32),
        in_specs=[smem] * 2 + [vmem] * 4 + [hbm] * 8,
        out_specs=vmem,
        scratch_shapes=[
            pltpu.VMEM(x.shape, jnp.bfloat16),
            pltpu.VMEM((chunks, users, CHUNK, prefix), jnp.bfloat16),
            pltpu.VMEM((chunks, users, prefix, CHUNK), jnp.bfloat16),
            pltpu.VMEM((chunks, routers, matrices, share, CHUNK), jnp.bfloat16),
            pltpu.VMEM((cores, matrices, share, width), jnp.bfloat16),
            pltpu.VMEM(w_one.shape, jnp.bfloat16),
            pltpu.VMEM((room, width), jnp.bfloat16),
            pltpu.VMEM((TILE, width), jnp.bfloat16),
            pltpu.VMEM((TILE, width), jnp.float32),
            pltpu.VMEM((TILE, width), jnp.float32),
            pltpu.VMEM((room, lanes), jnp.int32),
            pltpu.VMEM((room, lanes), jnp.float32),
            pltpu.VMEM((rows, lanes), jnp.float32),
            pltpu.SMEM((units,), jnp.int32),
            pltpu.SemaphoreType.DMA((1,)),
            pltpu.SemaphoreType.DMA((chunks, routers + 2)),
            pltpu.SemaphoreType.DMA((cores, routers)),
            pltpu.SemaphoreType.DMA((1,)),
        ],
        compiler_params=pltpu.CompilerParams(vmem_limit_bytes=VMEM_LIMIT),
        name="score_units",
        interpret=INTERPRET,
    )(codes, core, gain, gain2, mlp_gain, w_two, x, kt, kt2, values, values2, w, w2, w_one)


def local(
    items,
    block_owner,
    block_user,
    block_fill,
    prefix_keys,
    prefix_values,
    w_in,
    attn_gain,
    w_o,
    mlp_gain,
    w_one,
    w_two,
):
    blocks, block_width, model_width = items.shape
    peers = lax.axis_size("users")
    cores = lax.axis_size("heads")
    routers = lax.axis_size("routers")
    core = lax.axis_index("heads")
    flat_items = items.reshape(blocks * block_width, model_width)

    def swapped(x):
        return lax.ppermute(x, "heads", [(k, cores - 1 - k) for k in range(cores)])

    def exchanged(x):
        return lax.all_to_all(x, "users", split_axis=0, concat_axis=0, tiled=True)

    target = block_owner[:, 0]
    me = lax.axis_index("users")

    index = jnp.arange(blocks, dtype=jnp.int32)
    same = target[:, None] == target[None, :]
    ahead = (block_user[None, :] < block_user[:, None]) | (
        (block_user[None, :] == block_user[:, None]) & (index[None, :] < index[:, None])
    )
    packed_start = jnp.sum(jnp.where(same & ahead, block_fill[None, :], 0), axis=1)
    inside = lax.broadcasted_iota(jnp.int32, (blocks, block_width), 1)
    packed = packed_start[:, None] + inside
    here = (inside < block_fill[:, None]) & (packed % cores == core)
    goes_to = jnp.where(here, target[:, None] * block_width + packed // cores, -1)
    goes_to = goes_to.reshape(1, blocks * block_width)
    slot = lax.broadcasted_iota(jnp.int32, (peers * block_width, 1), 0)
    sent = jnp.dot(
        (slot == goes_to).astype(jnp.bfloat16), flat_items, preferred_element_type=jnp.float32
    ).astype(jnp.bfloat16)
    sent, block_user, w_in = lax.optimization_barrier((sent, block_user, w_in))
    arrived = exchanged(sent.reshape(peers, block_width, model_width))

    goes = target[None, :] == lax.broadcasted_iota(jnp.int32, (peers, blocks), 0)
    weight = jnp.where(block_user == 0, CODE + 1, 1) * block_fill
    every = jnp.sum(jnp.where(goes, weight[None, :], 0), axis=1)[None, :]

    def doubled(rows):
        step = rows.shape[0]
        if step >= peers:
            return rows
        pairs = [(k, (k + step) % peers) for k in range(peers)]
        return jnp.concatenate([rows, lax.ppermute(rows, "users", pairs)], axis=0)

    matrices, share, _ = w_in.shape
    w_local = jnp.concatenate([w_in, w_o.reshape(matrices, share, share)], axis=2)
    up = [(k, (k + 1) % routers) for k in range(routers)]
    down = [(k, (k - 1) % routers) for k in range(routers)]
    from_below, from_above = w_local, w_local
    ring = {0: w_local}
    for step in range(1, routers // 2):
        from_below = lax.ppermute(from_below, "routers", up)
        from_above = lax.ppermute(from_above, "routers", down)
        every = doubled(every)
        from_below, from_above, every = lax.optimization_barrier((from_below, from_above, every))
        ring[routers - step] = from_below
        ring[step] = from_above
    half = matrices // 2
    lower = lax.ppermute(from_below[:half], "routers", up)
    upper = lax.ppermute(from_above[half:], "routers", down)
    ring[routers // 2] = jnp.concatenate([lower, upper], axis=0)
    every = doubled(every)
    while every.shape[0] < peers:
        every = doubled(every)
    source = (me + peers - lax.broadcasted_iota(jnp.int32, (peers, peers, peers), 1)) % peers
    wanted = (source == lax.broadcasted_iota(jnp.int32, (peers, peers, peers), 0)) & (
        lax.broadcasted_iota(jnp.int32, (peers, peers, peers), 2) == me
    )
    codes = jnp.sum(jnp.where(wanted, every[None], 0), axis=(1, 2))
    w_ring = jnp.stack([ring[k] for k in range(routers)])
    own = (jnp.swapaxes(prefix_keys, 1, 2), prefix_values, attn_gain[None, :], w_ring)
    other = jax.tree.map(swapped, own)
    core_index = jnp.stack([core, lax.axis_index("routers")]).astype(jnp.int32)
    scores = score_units(
        codes, core_index, arrived, own, other, mlp_gain[None, :], w_one, w_two[None, :]
    ).reshape(peers, block_width)
    returned = exchanged(scores)
    returned = jnp.concatenate([returned, swapped(returned)], axis=1)
    row_scores = jnp.sum(jnp.where(goes[:, :, None], returned[:, None, :], 0.0), axis=0)
    lane = jnp.where(packed % cores == core, 0, block_width) + packed // cores
    wanted = lane[:, :, None] == lax.broadcasted_iota(
        jnp.int32, (blocks, block_width, cores * block_width), 2
    )
    block_scores = jnp.sum(jnp.where(wanted, row_scores[:, None, :], 0.0), axis=2)
    return jnp.where(inside < block_fill[:, None], block_scores, jnp.zeros_like(block_scores))


def solution(mesh):
    placed = (
        P(("groups", "users", "routers"), None, None),
        P(("groups", "users", "routers"), None),
        P(("groups", "users", "routers")),
        P(("groups", "users", "routers")),
        P(("groups", "users"), None, "heads"),
        P(("groups", "users"), None, "heads"),
        P(None, "routers", "heads"),
        P("heads"),
        P("heads", "routers"),
        P(),
        P(),
        P(),
    )
    return jax.shard_map(
        local,
        mesh=mesh,
        in_specs=placed,
        out_specs=P(("groups", "users", "routers"), None),
        check_vma=False,
    )
```

```python
import jax
import jax.numpy as jnp
from jax import lax
from jax.experimental import pallas as pl
from jax.experimental.pallas import tpu as pltpu
from jax.sharding import PartitionSpec as P


HEAD_DIM = 128
EPSILON = 1e-05
TILE = 256
CHUNK = 256
ALIGN = 16
CODE = 256


def half_silu(half):
    return half * (1.0 + jnp.tanh(half))


def score_kernel(
    code_ref,
    core_ref,
    gain_own,
    gain_other,
    mlp_gain_ref,
    w_two_ref,
    x_hbm,
    kt_own,
    kt_other,
    v_own,
    v_other,
    w_own,
    w_other,
    w_one_hbm,
    out_ref,
    x_ref,
    kt_ref,
    values_ref,
    w_ref,
    wo_ref,
    w_one_ref,
    rows_ref,
    prefix_ref,
    own_ref,
    gate_ref,
    user_ref,
    score_ref,
    unit_ref,
    offset_ref,
    row_sem,
    chunk_sem,
    wo_sem,
    one_sem,
):
    units, unit_rows, width = x_hbm.shape
    routers, _, share, _ = w_own.shape
    half_width = v_own.shape[2]
    cores = width // half_width
    per_side = half_width // CHUNK
    chunks = width // CHUNK
    scale = HEAD_DIM ** (-0.5)
    core = core_ref[0]
    router_here = core_ref[1]
    lanes = score_ref.shape[1]
    unit_row = lax.broadcasted_iota(jnp.int32, (unit_rows, lanes), 0)
    sides = ((kt_own, v_own, w_own), (kt_other, v_other, w_other))

    def ring_index(router):
        ahead = router - router_here
        return jnp.where(ahead < 0, ahead + routers, ahead)

    row_copy = pltpu.make_async_copy(x_hbm, x_ref, row_sem.at[0])
    row_copy.start()
    chunk_copies = []
    for chunk in range(chunks):
        kt, values, weights = sides[chunk // per_side]
        low = chunk % per_side * CHUNK
        copies = [
            pltpu.make_async_copy(
                weights.at[ring_index(router), :, :, low : low + CHUNK],
                w_ref.at[chunk, router],
                chunk_sem.at[chunk, router],
            )
            for router in range(routers)
        ]
        copies += [
            pltpu.make_async_copy(
                kt.at[:, low : low + CHUNK, :], kt_ref.at[chunk], chunk_sem.at[chunk, routers]
            ),
            pltpu.make_async_copy(
                values.at[:, :, low : low + CHUNK],
                values_ref.at[chunk],
                chunk_sem.at[chunk, routers + 1],
            ),
        ]
        for copy in copies:
            copy.start()
        chunk_copies.append(copies)
    tail_copies = []
    for side, (_, _, weights) in enumerate(sides):
        for router in range(routers):
            tail_copies.append(
                pltpu.make_async_copy(
                    weights.at[ring_index(router), :, :, half_width : half_width + share],
                    wo_ref.at[side, :, :, router * share : (router + 1) * share],
                    wo_sem.at[side, router],
                )
            )
    tail_copies.append(pltpu.make_async_copy(w_one_hbm, w_one_ref, one_sem.at[0]))
    for copy in tail_copies:
        copy.start()

    def rows_here(count):
        return (count + (cores - 1 - core)) // cores

    def place(unit, position):
        code = code_ref[unit]
        count = rows_here(code % CODE)
        first = rows_here(code // CODE)

        @pl.when(count > 0)
        def _():
            at = pl.multiple_of(position, ALIGN)
            rows_ref[pl.ds(at, unit_rows), :] = x_ref[unit]
            user_ref[pl.ds(at, unit_rows), :] = (unit_row >= first).astype(jnp.int32)

        offset_ref[unit] = position
        return position + (count + ALIGN - 1) // ALIGN * ALIGN

    row_copy.wait()
    total = lax.fori_loop(0, units, place, jnp.int32(0))

    def attend(user, queries, chunk, inner):
        raw = jnp.dot(
            queries,
            kt_ref[chunk, user, inner : inner + HEAD_DIM, :],
            preferred_element_type=jnp.float32,
        )
        weights = half_silu(raw * (0.5 * scale)).astype(jnp.bfloat16)
        return jnp.dot(
            weights,
            values_ref[chunk, user, :, inner : inner + HEAD_DIM],
            preferred_element_type=jnp.float32,
        )

    def tile_step(tile, wait):
        start = pl.multiple_of(tile * TILE, TILE)
        x = rows_ref[pl.ds(start, TILE), :]
        second = user_ref[pl.ds(start, TILE), :] > 0
        for chunk in range(chunks):
            at = chunk * CHUNK
            if wait:
                for copy in chunk_copies[chunk]:
                    copy.wait()

            def projected(which):
                weight = w_ref[chunk, :, which].reshape(width, CHUNK)
                return half_silu(jnp.dot(x, weight, preferred_element_type=jnp.float32) * 0.5)

            queries = projected(0).astype(jnp.bfloat16)
            keys = projected(1)
            values = projected(2)
            gate_ref[:, at : at + CHUNK] = projected(3)
            for inner in range(0, CHUNK, HEAD_DIM):
                part = slice(inner, inner + HEAD_DIM)
                place_at = slice(at + inner, at + inner + HEAD_DIM)
                raw = jnp.sum(
                    queries[:, part].astype(jnp.float32) * keys[:, part], axis=1, keepdims=True
                )
                own_ref[:, place_at] = half_silu(raw * (0.5 * scale)) * values[:, part]
                prefix_ref[:, place_at] = jnp.where(
                    second,
                    attend(1, queries[:, part], chunk, inner),
                    attend(0, queries[:, part], chunk, inner),
                ).astype(jnp.bfloat16)

        if wait:
            for copy in tail_copies:
                copy.wait()
        attended = prefix_ref[...].astype(jnp.float32) + own_ref[...]
        row_mean = jnp.sum(attended, axis=1, keepdims=True) / width
        row_var = jnp.sum(attended * attended, axis=1, keepdims=True) / width - row_mean * row_mean
        inverse = lax.rsqrt(row_var + EPSILON)
        residual = x.astype(jnp.float32)
        for side, gain_ref in enumerate((gain_own, gain_other)):
            part = slice(side * half_width, (side + 1) * half_width)
            gated = (
                (attended[:, part] - row_mean)
                * inverse
                * gain_ref[...].astype(jnp.float32)
                * gate_ref[:, part]
            ).astype(jnp.bfloat16)
            residual = residual + jnp.dot(
                gated,
                wo_ref[side].reshape(half_width, width),
                preferred_element_type=jnp.float32,
            )
        squares = jnp.sum(residual * residual, axis=1, keepdims=True)
        normed = (
            residual * lax.rsqrt(squares / width + EPSILON) * mlp_gain_ref[...].astype(jnp.float32)
        ).astype(jnp.bfloat16)
        inner_sum = jnp.dot(normed, w_one_ref[...], preferred_element_type=jnp.float32)
        hidden = half_silu(inner_sum * 0.5).astype(jnp.bfloat16).astype(jnp.float32)
        scores = jnp.sum(hidden * w_two_ref[...].astype(jnp.float32), axis=1, keepdims=True)
        score_ref[pl.ds(start, TILE), :] = jnp.broadcast_to(scores, (TILE, lanes))

    def later_tile(tile, carry):
        tile_step(tile, False)
        return carry

    tile_step(0, True)
    lax.fori_loop(1, (total + TILE - 1) // TILE, later_tile, 0)

    def unplace(unit, carry):
        count = rows_here(code_ref[unit] % CODE)
        to = pl.multiple_of(unit * unit_rows, unit_rows)

        @pl.when(count > 0)
        def _():
            at = pl.multiple_of(offset_ref[unit], ALIGN)
            found = score_ref[pl.ds(at, unit_rows), :]
            unit_ref[pl.ds(to, unit_rows), :] = jnp.where(unit_row < count, found, 0.0)

        @pl.when(count == 0)
        def _():
            unit_ref[pl.ds(to, unit_rows), :] = jnp.zeros((unit_rows, lanes), jnp.float32)

        return carry

    lax.fori_loop(0, units, unplace, 0)
    for block in range(units * unit_rows // lanes):
        out_ref[block : block + 1, :] = unit_ref[block * lanes : (block + 1) * lanes, :].T[0:1, :]


INTERPRET = False
VMEM_LIMIT = 40 * 1024 * 1024


def score_units(codes, core, x, own, other, mlp_gain, w_one, w_two):
    units, unit_rows, width = x.shape
    kt, values, gain, w = own
    kt2, values2, gain2, w2 = other
    users, prefix, half_width = values.shape
    routers, matrices, share, _ = w.shape
    cores = width // half_width
    chunks = width // CHUNK
    lanes = 128
    rows = units * unit_rows
    room = (rows + TILE - 1) // TILE * TILE + max(TILE, unit_rows)
    smem = pl.BlockSpec(memory_space=pltpu.SMEM)
    vmem = pl.BlockSpec(memory_space=pltpu.VMEM)
    hbm = pl.BlockSpec(memory_space=pltpu.HBM)
    return pl.pallas_call(
        score_kernel,
        out_shape=jax.ShapeDtypeStruct((rows // lanes, lanes), jnp.float32),
        in_specs=[smem] * 2 + [vmem] * 4 + [hbm] * 8,
        out_specs=vmem,
        scratch_shapes=[
            pltpu.VMEM(x.shape, jnp.bfloat16),
            pltpu.VMEM((chunks, users, CHUNK, prefix), jnp.bfloat16),
            pltpu.VMEM((chunks, users, prefix, CHUNK), jnp.bfloat16),
            pltpu.VMEM((chunks, routers, matrices, share, CHUNK), jnp.bfloat16),
            pltpu.VMEM((cores, matrices, share, width), jnp.bfloat16),
            pltpu.VMEM(w_one.shape, jnp.bfloat16),
            pltpu.VMEM((room, width), jnp.bfloat16),
            pltpu.VMEM((TILE, width), jnp.bfloat16),
            pltpu.VMEM((TILE, width), jnp.float32),
            pltpu.VMEM((TILE, width), jnp.float32),
            pltpu.VMEM((room, lanes), jnp.int32),
            pltpu.VMEM((room, lanes), jnp.float32),
            pltpu.VMEM((rows, lanes), jnp.float32),
            pltpu.SMEM((units,), jnp.int32),
            pltpu.SemaphoreType.DMA((1,)),
            pltpu.SemaphoreType.DMA((chunks, routers + 2)),
            pltpu.SemaphoreType.DMA((cores, routers)),
            pltpu.SemaphoreType.DMA((1,)),
        ],
        compiler_params=pltpu.CompilerParams(vmem_limit_bytes=VMEM_LIMIT),
        name="score_units",
        interpret=INTERPRET,
    )(codes, core, gain, gain2, mlp_gain, w_two, x, kt, kt2, values, values2, w, w2, w_one)


def local(
    items,
    block_owner,
    block_user,
    block_fill,
    prefix_keys,
    prefix_values,
    w_in,
    attn_gain,
    w_o,
    mlp_gain,
    w_one,
    w_two,
):
    blocks, block_width, model_width = items.shape
    peers = lax.axis_size("users")
    cores = lax.axis_size("heads")
    routers = lax.axis_size("routers")
    core = lax.axis_index("heads")
    flat_items = items.reshape(blocks * block_width, model_width)

    def swapped(x):
        return lax.ppermute(x, "heads", [(k, cores - 1 - k) for k in range(cores)])

    def exchanged(x):
        return lax.all_to_all(x, "users", split_axis=0, concat_axis=0, tiled=True)

    target = block_owner[:, 0]
    goes = target[None, :] == lax.broadcasted_iota(jnp.int32, (peers, blocks), 0)
    weight = jnp.where(block_user == 0, CODE + 1, 1) * block_fill
    codes = jnp.sum(jnp.where(goes, weight[None, :], 0), axis=1)
    codes = exchanged(codes.reshape(peers, 1)).reshape(peers)

    index = jnp.arange(blocks, dtype=jnp.int32)
    same = target[:, None] == target[None, :]
    ahead = (block_user[None, :] < block_user[:, None]) | (
        (block_user[None, :] == block_user[:, None]) & (index[None, :] < index[:, None])
    )
    packed_start = jnp.sum(jnp.where(same & ahead, block_fill[None, :], 0), axis=1)
    inside = lax.broadcasted_iota(jnp.int32, (blocks, block_width), 1)
    packed = packed_start[:, None] + inside
    here = (inside < block_fill[:, None]) & (packed % cores == core)
    goes_to = jnp.where(here, target[:, None] * block_width + packed // cores, -1)
    goes_to = goes_to.reshape(1, blocks * block_width)
    slot = lax.broadcasted_iota(jnp.int32, (peers * block_width, 1), 0)
    sent = jnp.dot(
        (slot == goes_to).astype(jnp.bfloat16), flat_items, preferred_element_type=jnp.float32
    ).astype(jnp.bfloat16)
    sent, w_in = lax.optimization_barrier((sent, w_in))
    arrived = exchanged(sent.reshape(peers, block_width, model_width))

    matrices, share, _ = w_in.shape
    w_local = jnp.concatenate([w_in, w_o.reshape(matrices, share, share)], axis=2)
    up = [(k, (k + 1) % routers) for k in range(routers)]
    down = [(k, (k - 1) % routers) for k in range(routers)]
    from_below, from_above = w_local, w_local
    ring = {0: w_local}
    for step in range(1, routers // 2):
        from_below = lax.ppermute(from_below, "routers", up)
        from_above = lax.ppermute(from_above, "routers", down)
        ring[routers - step] = from_below
        ring[step] = from_above
    half = matrices // 2
    lower = lax.ppermute(from_below[:half], "routers", up)
    upper = lax.ppermute(from_above[half:], "routers", down)
    ring[routers // 2] = jnp.concatenate([lower, upper], axis=0)
    w_ring = jnp.stack([ring[k] for k in range(routers)])
    own = (jnp.swapaxes(prefix_keys, 1, 2), prefix_values, attn_gain[None, :], w_ring)
    other = jax.tree.map(swapped, own)
    core_index = jnp.stack([core, lax.axis_index("routers")]).astype(jnp.int32)
    scores = score_units(
        codes, core_index, arrived, own, other, mlp_gain[None, :], w_one, w_two[None, :]
    ).reshape(peers, block_width)
    back = jnp.broadcast_to(scores[:, None, :], (peers, cores, block_width))
    returned = lax.all_to_all(
        back.reshape(peers * cores, block_width),
        ("users", "heads"),
        split_axis=0,
        concat_axis=0,
        tiled=True,
    ).reshape(peers, cores * block_width)
    row_scores = jnp.sum(jnp.where(goes[:, :, None], returned[:, None, :], 0.0), axis=0)
    lane = packed % cores * block_width + packed // cores
    wanted = lane[:, :, None] == lax.broadcasted_iota(
        jnp.int32, (blocks, block_width, cores * block_width), 2
    )
    block_scores = jnp.sum(jnp.where(wanted, row_scores[:, None, :], 0.0), axis=2)
    return jnp.where(inside < block_fill[:, None], block_scores, jnp.zeros_like(block_scores))


def solution(mesh):
    placed = (
        P(("groups", "users", "routers"), None, None),
        P(("groups", "users", "routers"), None),
        P(("groups", "users", "routers")),
        P(("groups", "users", "routers")),
        P(("groups", "users"), None, "heads"),
        P(("groups", "users"), None, "heads"),
        P(None, "routers", "heads"),
        P("heads"),
        P("heads", "routers"),
        P(),
        P(),
        P(),
    )
    return jax.shard_map(
        local,
        mesh=mesh,
        in_specs=placed,
        out_specs=P(("groups", "users", "routers"), None),
        check_vma=False,
    )
```

```python
import jax
import jax.numpy as jnp
from jax import lax
from jax.experimental import pallas as pl
from jax.experimental.pallas import tpu as pltpu
from jax.sharding import PartitionSpec as P


HEAD_DIM = 128
EPSILON = 1e-05
TILE = 256
CHUNK = 256
ALIGN = 16
CODE = 128
UNUSED = 200.0
HEADER = 64.0
LOW = 32.0
HIGH = 4096.0
TINY = 2.0**-110
TINY_MARK = 2.0**14
LIFT = 2.0**125


def half_silu(half):
    return half * (1.0 + jnp.tanh(half))


def marked(rows, count, first):
    slots = rows.shape[1]
    slot = lax.broadcasted_iota(jnp.int32, rows.shape, 1)
    lane = lax.broadcasted_iota(jnp.int32, rows.shape, 2)
    count = count[:, None, None]
    first = first[:, None, None]
    last = slot == slots - 1
    unused = jnp.where(last, HEADER + first.astype(jnp.float32), UNUSED)
    lifted = jnp.where(jnp.abs(rows) < TINY, TINY_MARK, rows * LIFT)
    full = last & (count == slots)
    lift = full & (((lane == 0) & (first > 0)) | ((lane == 1) & (first == slots)))
    return jnp.where((slot >= count) & (lane == 0), unused, jnp.where(lift, lifted, rows))


def code_of(head):
    slots = head.shape[0]
    slot = lax.broadcasted_iota(jnp.int32, head.shape, 0)
    lane = lax.broadcasted_iota(jnp.int32, head.shape, 1)
    size = jnp.abs(head)
    valid = (size < LOW) | (size > HIGH)
    last = slot == slots - 1
    counts = jnp.where((lane == 0) & valid, 1.0, 0.0)
    header = jnp.where(last & (lane == 0) & ~valid, head - HEADER, 0.0)
    lifted = jnp.where(last & (lane <= 1) & (size > HIGH), slots / 2.0, 0.0)
    return jnp.sum(counts + CODE * (header + lifted))


def unmarked(rows):
    size = jnp.abs(rows)
    lowered = jnp.where(size < 2.0 * TINY_MARK, 0.0, rows * (1.0 / LIFT))
    return jnp.where(size > HIGH, lowered, rows)


def score_kernel(
    core_ref,
    gain_own,
    gain_other,
    mlp_gain_ref,
    w_two_ref,
    x_hbm,
    kt_own,
    kt_other,
    v_own,
    v_other,
    w_own,
    w_other,
    w_one_hbm,
    out_ref,
    x_ref,
    kt_ref,
    values_ref,
    w_ref,
    wo_ref,
    w_one_ref,
    rows_ref,
    prefix_ref,
    own_ref,
    gate_ref,
    user_ref,
    score_ref,
    unit_ref,
    offset_ref,
    code_ref,
    row_sem,
    chunk_sem,
    wo_sem,
    one_sem,
):
    units, unit_rows, width = x_hbm.shape
    routers, _, share, _ = w_own.shape
    half_width = v_own.shape[2]
    per_side = half_width // CHUNK
    chunks = width // CHUNK
    scale = HEAD_DIM ** (-0.5)
    router_here = core_ref[0]
    lanes = score_ref.shape[1]
    unit_row = lax.broadcasted_iota(jnp.int32, (unit_rows, lanes), 0)
    sides = ((kt_own, v_own, w_own), (kt_other, v_other, w_other))

    def ring_index(router):
        ahead = router - router_here
        return jnp.where(ahead < 0, ahead + routers, ahead)

    row_copy = pltpu.make_async_copy(x_hbm, x_ref, row_sem.at[0])
    row_copy.start()
    chunk_copies = []
    for chunk in range(chunks):
        kt, values, weights = sides[chunk // per_side]
        low = chunk % per_side * CHUNK
        copies = [
            pltpu.make_async_copy(
                weights.at[ring_index(router), :, :, low : low + CHUNK],
                w_ref.at[chunk, router],
                chunk_sem.at[chunk, router],
            )
            for router in range(routers)
        ]
        copies += [
            pltpu.make_async_copy(
                kt.at[:, low : low + CHUNK, :], kt_ref.at[chunk], chunk_sem.at[chunk, routers]
            ),
            pltpu.make_async_copy(
                values.at[:, :, low : low + CHUNK],
                values_ref.at[chunk],
                chunk_sem.at[chunk, routers + 1],
            ),
        ]
        for copy in copies:
            copy.start()
        chunk_copies.append(copies)
    tail_copies = []
    for side, (_, _, weights) in enumerate(sides):
        for router in range(routers):
            tail_copies.append(
                pltpu.make_async_copy(
                    weights.at[ring_index(router), :, :, half_width : half_width + share],
                    wo_ref.at[side, :, :, router * share : (router + 1) * share],
                    wo_sem.at[side, router],
                )
            )
    tail_copies.append(pltpu.make_async_copy(w_one_hbm, w_one_ref, one_sem.at[0]))
    for copy in tail_copies:
        copy.start()

    def place(unit, position):
        code = code_ref[unit]
        count = code % CODE
        first = code // CODE

        @pl.when(count > 0)
        def _():
            at = pl.multiple_of(position, ALIGN)
            rows_ref[pl.ds(at, unit_rows), :] = x_ref[unit]
            user_ref[pl.ds(at, unit_rows), :] = (unit_row >= first).astype(jnp.int32)

        offset_ref[unit] = position
        return position + (count + ALIGN - 1) // ALIGN * ALIGN

    row_copy.wait()
    for unit in range(units):
        head = x_ref[unit, :, 0:lanes].astype(jnp.float32)
        code_ref[unit] = code_of(head).astype(jnp.int32)
        x_ref[unit, :, 0:lanes] = unmarked(head).astype(jnp.bfloat16)
    total = lax.fori_loop(0, units, place, jnp.int32(0))

    def attend(user, queries, chunk, inner):
        raw = jnp.dot(
            queries,
            kt_ref[chunk, user, inner : inner + HEAD_DIM, :],
            preferred_element_type=jnp.float32,
        )
        weights = half_silu(raw * (0.5 * scale)).astype(jnp.bfloat16)
        return jnp.dot(
            weights,
            values_ref[chunk, user, :, inner : inner + HEAD_DIM],
            preferred_element_type=jnp.float32,
        )

    def tile_step(tile, wait):
        start = pl.multiple_of(tile * TILE, TILE)
        x = rows_ref[pl.ds(start, TILE), :]
        second = user_ref[pl.ds(start, TILE), :] > 0
        for chunk in range(chunks):
            at = chunk * CHUNK
            if wait:
                for copy in chunk_copies[chunk]:
                    copy.wait()

            def projected(which):
                weight = w_ref[chunk, :, which].reshape(width, CHUNK)
                return half_silu(jnp.dot(x, weight, preferred_element_type=jnp.float32) * 0.5)

            queries = projected(0).astype(jnp.bfloat16)
            keys = projected(1)
            values = projected(2)
            gate_ref[:, at : at + CHUNK] = projected(3)
            for inner in range(0, CHUNK, HEAD_DIM):
                part = slice(inner, inner + HEAD_DIM)
                place_at = slice(at + inner, at + inner + HEAD_DIM)
                raw = jnp.sum(
                    queries[:, part].astype(jnp.float32) * keys[:, part], axis=1, keepdims=True
                )
                own_ref[:, place_at] = half_silu(raw * (0.5 * scale)) * values[:, part]
                prefix_ref[:, place_at] = jnp.where(
                    second,
                    attend(1, queries[:, part], chunk, inner),
                    attend(0, queries[:, part], chunk, inner),
                ).astype(jnp.bfloat16)

        if wait:
            for copy in tail_copies:
                copy.wait()
        attended = prefix_ref[...].astype(jnp.float32) + own_ref[...]
        row_mean = jnp.sum(attended, axis=1, keepdims=True) / width
        row_var = jnp.sum(attended * attended, axis=1, keepdims=True) / width - row_mean * row_mean
        inverse = lax.rsqrt(row_var + EPSILON)
        residual = x.astype(jnp.float32)
        for side, gain_ref in enumerate((gain_own, gain_other)):
            part = slice(side * half_width, (side + 1) * half_width)
            gated = (
                (attended[:, part] - row_mean)
                * inverse
                * gain_ref[...].astype(jnp.float32)
                * gate_ref[:, part]
            ).astype(jnp.bfloat16)
            residual = residual + jnp.dot(
                gated,
                wo_ref[side].reshape(half_width, width),
                preferred_element_type=jnp.float32,
            )
        squares = jnp.sum(residual * residual, axis=1, keepdims=True)
        normed = (
            residual * lax.rsqrt(squares / width + EPSILON) * mlp_gain_ref[...].astype(jnp.float32)
        ).astype(jnp.bfloat16)
        inner_sum = jnp.dot(normed, w_one_ref[...], preferred_element_type=jnp.float32)
        hidden = half_silu(inner_sum * 0.5).astype(jnp.bfloat16).astype(jnp.float32)
        scores = jnp.sum(hidden * w_two_ref[...].astype(jnp.float32), axis=1, keepdims=True)
        score_ref[pl.ds(start, TILE), :] = jnp.broadcast_to(scores, (TILE, lanes))

    def later_tile(tile, carry):
        tile_step(tile, False)
        return carry

    tile_step(0, True)
    lax.fori_loop(1, (total + TILE - 1) // TILE, later_tile, 0)

    def unplace(unit, carry):
        count = code_ref[unit] % CODE
        to = pl.multiple_of(unit * unit_rows, unit_rows)

        @pl.when(count > 0)
        def _():
            at = pl.multiple_of(offset_ref[unit], ALIGN)
            found = score_ref[pl.ds(at, unit_rows), :]
            unit_ref[pl.ds(to, unit_rows), :] = jnp.where(unit_row < count, found, 0.0)

        @pl.when(count == 0)
        def _():
            unit_ref[pl.ds(to, unit_rows), :] = jnp.zeros((unit_rows, lanes), jnp.float32)

        return carry

    lax.fori_loop(0, units, unplace, 0)
    for block in range(units * unit_rows // lanes):
        out_ref[block : block + 1, :] = unit_ref[block * lanes : (block + 1) * lanes, :].T[0:1, :]


INTERPRET = False
VMEM_LIMIT = 40 * 1024 * 1024


def score_units(place_here, x, own, other, mlp_gain, w_one, w_two):
    units, unit_rows, width = x.shape
    kt, values, gain, w = own
    kt2, values2, gain2, w2 = other
    users, prefix, half_width = values.shape
    routers, matrices, share, _ = w.shape
    cores = width // half_width
    chunks = width // CHUNK
    lanes = 128
    rows = units * unit_rows
    room = (rows + TILE - 1) // TILE * TILE + max(TILE, unit_rows)
    smem = pl.BlockSpec(memory_space=pltpu.SMEM)
    vmem = pl.BlockSpec(memory_space=pltpu.VMEM)
    hbm = pl.BlockSpec(memory_space=pltpu.HBM)
    return pl.pallas_call(
        score_kernel,
        out_shape=jax.ShapeDtypeStruct((rows // lanes, lanes), jnp.float32),
        in_specs=[smem] + [vmem] * 4 + [hbm] * 8,
        out_specs=vmem,
        scratch_shapes=[
            pltpu.VMEM(x.shape, jnp.bfloat16),
            pltpu.VMEM((chunks, users, CHUNK, prefix), jnp.bfloat16),
            pltpu.VMEM((chunks, users, prefix, CHUNK), jnp.bfloat16),
            pltpu.VMEM((chunks, routers, matrices, share, CHUNK), jnp.bfloat16),
            pltpu.VMEM((cores, matrices, share, width), jnp.bfloat16),
            pltpu.VMEM(w_one.shape, jnp.bfloat16),
            pltpu.VMEM((room, width), jnp.bfloat16),
            pltpu.VMEM((TILE, width), jnp.bfloat16),
            pltpu.VMEM((TILE, width), jnp.float32),
            pltpu.VMEM((TILE, width), jnp.float32),
            pltpu.VMEM((room, lanes), jnp.int32),
            pltpu.VMEM((room, lanes), jnp.float32),
            pltpu.VMEM((rows, lanes), jnp.float32),
            pltpu.SMEM((units,), jnp.int32),
            pltpu.SMEM((units,), jnp.int32),
            pltpu.SemaphoreType.DMA((1,)),
            pltpu.SemaphoreType.DMA((chunks, routers + 2)),
            pltpu.SemaphoreType.DMA((cores, routers)),
            pltpu.SemaphoreType.DMA((1,)),
        ],
        compiler_params=pltpu.CompilerParams(vmem_limit_bytes=VMEM_LIMIT),
        name="score_units",
        interpret=INTERPRET,
    )(place_here, gain, gain2, mlp_gain, w_two, x, kt, kt2, values, values2, w, w2, w_one)


def local(
    items,
    block_owner,
    block_user,
    block_fill,
    prefix_keys,
    prefix_values,
    w_in,
    attn_gain,
    w_o,
    mlp_gain,
    w_one,
    w_two,
):
    blocks, block_width, model_width = items.shape
    peers = lax.axis_size("users")
    cores = lax.axis_size("heads")
    routers = lax.axis_size("routers")
    core = lax.axis_index("heads")
    flat_items = items.reshape(blocks * block_width, model_width)

    def swapped(x):
        return lax.ppermute(x, "heads", [(k, cores - 1 - k) for k in range(cores)])

    def exchanged(x):
        return lax.all_to_all(x, "users", split_axis=0, concat_axis=0, tiled=True)

    target = block_owner[:, 0]
    goes = target[None, :] == lax.broadcasted_iota(jnp.int32, (peers, blocks), 0)

    def rows_here(chosen):
        rows = jnp.sum(jnp.where(goes & chosen[None, :], block_fill[None, :], 0), axis=1)
        return (rows + (cores - 1 - core)) // cores

    index = jnp.arange(blocks, dtype=jnp.int32)
    same = target[:, None] == target[None, :]
    ahead = (block_user[None, :] < block_user[:, None]) | (
        (block_user[None, :] == block_user[:, None]) & (index[None, :] < index[:, None])
    )
    packed_start = jnp.sum(jnp.where(same & ahead, block_fill[None, :], 0), axis=1)
    inside = lax.broadcasted_iota(jnp.int32, (blocks, block_width), 1)
    packed = packed_start[:, None] + inside
    here = (inside < block_fill[:, None]) & (packed % cores == core)
    goes_to = jnp.where(here, target[:, None] * block_width + packed // cores, -1)
    goes_to = goes_to.reshape(1, blocks * block_width)
    slot = lax.broadcasted_iota(jnp.int32, (peers * block_width, 1), 0)
    sent = jnp.dot(
        (slot == goes_to).astype(jnp.bfloat16), flat_items, preferred_element_type=jnp.float32
    ).reshape(peers, block_width, model_width)
    sent = marked(sent, rows_here(block_user >= 0), rows_here(block_user == 0)).astype(jnp.bfloat16)
    sent, w_in = lax.optimization_barrier((sent, w_in))
    arrived = exchanged(sent)

    matrices, share, _ = w_in.shape
    w_local = jnp.concatenate([w_in, w_o.reshape(matrices, share, share)], axis=2)
    up = [(k, (k + 1) % routers) for k in range(routers)]
    down = [(k, (k - 1) % routers) for k in range(routers)]
    from_below, from_above = w_local, w_local
    ring = {0: w_local}
    for step in range(1, routers // 2):
        from_below = lax.ppermute(from_below, "routers", up)
        from_above = lax.ppermute(from_above, "routers", down)
        ring[routers - step] = from_below
        ring[step] = from_above
    half = matrices // 2
    lower = lax.ppermute(from_below[:half], "routers", up)
    upper = lax.ppermute(from_above[half:], "routers", down)
    ring[routers // 2] = jnp.concatenate([lower, upper], axis=0)
    w_ring = jnp.stack([ring[k] for k in range(routers)])
    own = (jnp.swapaxes(prefix_keys, 1, 2), prefix_values, attn_gain[None, :], w_ring)
    other = jax.tree.map(swapped, own)
    place_here = lax.axis_index("routers").astype(jnp.int32).reshape(1)
    scores = score_units(
        place_here, arrived, own, other, mlp_gain[None, :], w_one, w_two[None, :]
    ).reshape(peers, block_width)
    back = jnp.broadcast_to(scores[:, None, :], (peers, cores, block_width))
    returned = lax.all_to_all(
        back.reshape(peers * cores, block_width),
        ("users", "heads"),
        split_axis=0,
        concat_axis=0,
        tiled=True,
    ).reshape(peers, cores * block_width)
    row_scores = jnp.sum(jnp.where(goes[:, :, None], returned[:, None, :], 0.0), axis=0)
    lane = packed % cores * block_width + packed // cores
    wanted = lane[:, :, None] == lax.broadcasted_iota(
        jnp.int32, (blocks, block_width, cores * block_width), 2
    )
    block_scores = jnp.sum(jnp.where(wanted, row_scores[:, None, :], 0.0), axis=2)
    return jnp.where(inside < block_fill[:, None], block_scores, jnp.zeros_like(block_scores))


def solution(mesh):
    placed = (
        P(("groups", "users", "routers"), None, None),
        P(("groups", "users", "routers"), None),
        P(("groups", "users", "routers")),
        P(("groups", "users", "routers")),
        P(("groups", "users"), None, "heads"),
        P(("groups", "users"), None, "heads"),
        P(None, "routers", "heads"),
        P("heads"),
        P("heads", "routers"),
        P(),
        P(),
        P(),
    )
    return jax.shard_map(
        local,
        mesh=mesh,
        in_specs=placed,
        out_specs=P(("groups", "users", "routers"), None),
        check_vma=False,
    )
```

```python
import jax
import jax.numpy as jnp
from jax import lax
from jax.experimental import pallas as pl
from jax.experimental.pallas import tpu as pltpu
from jax.sharding import PartitionSpec as P


HEAD_DIM = 128
EPSILON = 1e-05
TILE = 256
CHUNK = 256
ALIGN = 16
CODE = 128
UNUSED = 200.0
HEADER = 64.0
LOW = 32.0
HIGH = 4096.0
TINY = 2.0**-110
TINY_MARK = 2.0**14
LIFT = 2.0**125


def half_silu(half):
    return half * (1.0 + jnp.tanh(half))


def marked(rows, count, first):
    slots = rows.shape[1]
    slot = lax.broadcasted_iota(jnp.int32, rows.shape, 1)
    lane = lax.broadcasted_iota(jnp.int32, rows.shape, 2)
    count = count[:, None, None]
    first = first[:, None, None]
    last = slot == slots - 1
    unused = jnp.where(last, HEADER + first.astype(jnp.float32), UNUSED)
    lifted = jnp.where(jnp.abs(rows) < TINY, TINY_MARK, rows * LIFT)
    full = last & (count == slots)
    lift = full & (((lane == 0) & (first > 0)) | ((lane == 1) & (first == slots)))
    return jnp.where((slot >= count) & (lane == 0), unused, jnp.where(lift, lifted, rows))


def code_of(head):
    slots = head.shape[0]
    slot = lax.broadcasted_iota(jnp.int32, head.shape, 0)
    lane = lax.broadcasted_iota(jnp.int32, head.shape, 1)
    size = jnp.abs(head)
    valid = (size < LOW) | (size > HIGH)
    last = slot == slots - 1
    counts = jnp.where((lane == 0) & valid, 1.0, 0.0)
    header = jnp.where(last & (lane == 0) & ~valid, head - HEADER, 0.0)
    lifted = jnp.where(last & (lane <= 1) & (size > HIGH), slots / 2.0, 0.0)
    return jnp.sum(counts + CODE * (header + lifted))


def unmarked(rows):
    size = jnp.abs(rows)
    lowered = jnp.where(size < 2.0 * TINY_MARK, 0.0, rows * (1.0 / LIFT))
    return jnp.where(size > HIGH, lowered, rows)


def score_kernel(
    core_ref,
    gain_own,
    gain_other,
    mlp_gain_ref,
    w_two_ref,
    x_hbm,
    kt_own,
    kt_other,
    v_own,
    v_other,
    w_own,
    w_other,
    w_one_hbm,
    out_ref,
    x_ref,
    kt_ref,
    values_ref,
    w_ref,
    wo_ref,
    w_one_ref,
    rows_ref,
    prefix_ref,
    own_ref,
    gate_ref,
    user_ref,
    score_ref,
    unit_ref,
    offset_ref,
    code_ref,
    row_sem,
    chunk_sem,
    wo_sem,
    one_sem,
):
    units, unit_rows, width = x_hbm.shape
    routers, _, share, _ = w_own.shape
    half_width = v_own.shape[2]
    per_side = half_width // CHUNK
    chunks = width // CHUNK
    scale = HEAD_DIM ** (-0.5)
    router_here = core_ref[0]
    lanes = score_ref.shape[1]
    unit_row = lax.broadcasted_iota(jnp.int32, (unit_rows, lanes), 0)
    sides = ((kt_own, v_own, w_own), (kt_other, v_other, w_other))

    def ring_index(router):
        ahead = router - router_here
        return jnp.where(ahead < 0, ahead + routers, ahead)

    row_copy = pltpu.make_async_copy(x_hbm, x_ref, row_sem.at[0])
    row_copy.start()
    chunk_copies = []
    for chunk in range(chunks):
        kt, values, weights = sides[chunk // per_side]
        low = chunk % per_side * CHUNK
        copies = [
            pltpu.make_async_copy(
                weights.at[ring_index(router), :, :, low : low + CHUNK],
                w_ref.at[chunk, router],
                chunk_sem.at[chunk, router],
            )
            for router in range(routers)
        ]
        copies += [
            pltpu.make_async_copy(
                kt.at[:, low : low + CHUNK, :], kt_ref.at[chunk], chunk_sem.at[chunk, routers]
            ),
            pltpu.make_async_copy(
                values.at[:, :, low : low + CHUNK],
                values_ref.at[chunk],
                chunk_sem.at[chunk, routers + 1],
            ),
        ]
        for copy in copies:
            copy.start()
        chunk_copies.append(copies)
    tail_copies = []
    for side, (_, _, weights) in enumerate(sides):
        for router in range(routers):
            tail_copies.append(
                pltpu.make_async_copy(
                    weights.at[ring_index(router), :, :, half_width : half_width + share],
                    wo_ref.at[side, :, :, router * share : (router + 1) * share],
                    wo_sem.at[side, router],
                )
            )
    tail_copies.append(pltpu.make_async_copy(w_one_hbm, w_one_ref, one_sem.at[0]))
    for copy in tail_copies:
        copy.start()

    def place(unit, position):
        code = code_ref[unit]
        count = code % CODE
        first = code // CODE

        @pl.when(count > 0)
        def _():
            at = pl.multiple_of(position, ALIGN)
            rows_ref[pl.ds(at, unit_rows), :] = x_ref[unit]
            user_ref[pl.ds(at, unit_rows), :] = (unit_row >= first).astype(jnp.int32)

        offset_ref[unit] = position
        return position + (count + ALIGN - 1) // ALIGN * ALIGN

    row_copy.wait()
    for unit in range(units):
        head = x_ref[unit, :, 0:lanes].astype(jnp.float32)
        code_ref[unit] = code_of(head).astype(jnp.int32)
        x_ref[unit, :, 0:lanes] = unmarked(head).astype(jnp.bfloat16)
    total = lax.fori_loop(0, units, place, jnp.int32(0))

    def attend(user, queries, chunk, inner):
        raw = jnp.dot(
            queries,
            kt_ref[chunk, user, inner : inner + HEAD_DIM, :],
            preferred_element_type=jnp.float32,
        )
        weights = half_silu(raw * (0.5 * scale)).astype(jnp.bfloat16)
        return jnp.dot(
            weights,
            values_ref[chunk, user, :, inner : inner + HEAD_DIM],
            preferred_element_type=jnp.float32,
        )

    def tile_step(tile, wait):
        start = pl.multiple_of(tile * TILE, TILE)
        x = rows_ref[pl.ds(start, TILE), :]
        second = user_ref[pl.ds(start, TILE), :] > 0
        for chunk in range(chunks):
            at = chunk * CHUNK
            if wait:
                for copy in chunk_copies[chunk]:
                    copy.wait()

            def projected(which):
                weight = w_ref[chunk, :, which].reshape(width, CHUNK)
                return half_silu(jnp.dot(x, weight, preferred_element_type=jnp.float32) * 0.5)

            queries = projected(0).astype(jnp.bfloat16)
            keys = projected(1)
            values = projected(2)
            gate_ref[:, at : at + CHUNK] = projected(3)
            for inner in range(0, CHUNK, HEAD_DIM):
                part = slice(inner, inner + HEAD_DIM)
                place_at = slice(at + inner, at + inner + HEAD_DIM)
                raw = jnp.sum(
                    queries[:, part].astype(jnp.float32) * keys[:, part], axis=1, keepdims=True
                )
                own_ref[:, place_at] = half_silu(raw * (0.5 * scale)) * values[:, part]
                prefix_ref[:, place_at] = jnp.where(
                    second,
                    attend(1, queries[:, part], chunk, inner),
                    attend(0, queries[:, part], chunk, inner),
                ).astype(jnp.bfloat16)

        if wait:
            for copy in tail_copies:
                copy.wait()
        attended = prefix_ref[...].astype(jnp.float32) + own_ref[...]
        row_mean = jnp.sum(attended, axis=1, keepdims=True) / width
        row_var = jnp.sum(attended * attended, axis=1, keepdims=True) / width - row_mean * row_mean
        inverse = lax.rsqrt(row_var + EPSILON)
        residual = x.astype(jnp.float32)
        for side, gain_ref in enumerate((gain_own, gain_other)):
            part = slice(side * half_width, (side + 1) * half_width)
            gated = (
                (attended[:, part] - row_mean)
                * inverse
                * gain_ref[...].astype(jnp.float32)
                * gate_ref[:, part]
            ).astype(jnp.bfloat16)
            residual = residual + jnp.dot(
                gated,
                wo_ref[side].reshape(half_width, width),
                preferred_element_type=jnp.float32,
            )
        squares = jnp.sum(residual * residual, axis=1, keepdims=True)
        normed = (
            residual * lax.rsqrt(squares / width + EPSILON) * mlp_gain_ref[...].astype(jnp.float32)
        ).astype(jnp.bfloat16)
        inner_sum = jnp.dot(normed, w_one_ref[...], preferred_element_type=jnp.float32)
        hidden = half_silu(inner_sum * 0.5).astype(jnp.bfloat16).astype(jnp.float32)
        scores = jnp.sum(hidden * w_two_ref[...].astype(jnp.float32), axis=1, keepdims=True)
        score_ref[pl.ds(start, TILE), :] = jnp.broadcast_to(scores, (TILE, lanes))

    def later_tile(tile, carry):
        tile_step(tile, False)
        return carry

    tile_step(0, True)
    lax.fori_loop(1, (total + TILE - 1) // TILE, later_tile, 0)

    def unplace(unit, carry):
        count = code_ref[unit] % CODE
        to = pl.multiple_of(unit * unit_rows, unit_rows)

        @pl.when(count > 0)
        def _():
            at = pl.multiple_of(offset_ref[unit], ALIGN)
            found = score_ref[pl.ds(at, unit_rows), :]
            unit_ref[pl.ds(to, unit_rows), :] = jnp.where(unit_row < count, found, 0.0)

        @pl.when(count == 0)
        def _():
            unit_ref[pl.ds(to, unit_rows), :] = jnp.zeros((unit_rows, lanes), jnp.float32)

        return carry

    lax.fori_loop(0, units, unplace, 0)
    square = (lanes, lanes)
    diagonal = lax.broadcasted_iota(jnp.int32, square, 0) == lax.broadcasted_iota(
        jnp.int32, square, 1
    )
    for block in range(units * unit_rows // lanes):
        rows = unit_ref[block * lanes : (block + 1) * lanes, :]
        out_ref[block : block + 1, :] = jnp.sum(
            jnp.where(diagonal, rows, 0.0), axis=0, keepdims=True
        )


INTERPRET = False
VMEM_LIMIT = 40 * 1024 * 1024


def score_units(place_here, x, own, other, mlp_gain, w_one, w_two):
    units, unit_rows, width = x.shape
    kt, values, gain, w = own
    kt2, values2, gain2, w2 = other
    users, prefix, half_width = values.shape
    routers, matrices, share, _ = w.shape
    cores = width // half_width
    chunks = width // CHUNK
    lanes = 128
    rows = units * unit_rows
    room = (rows + TILE - 1) // TILE * TILE + max(TILE, unit_rows)
    smem = pl.BlockSpec(memory_space=pltpu.SMEM)
    vmem = pl.BlockSpec(memory_space=pltpu.VMEM)
    hbm = pl.BlockSpec(memory_space=pltpu.HBM)
    return pl.pallas_call(
        score_kernel,
        out_shape=jax.ShapeDtypeStruct((rows // lanes, lanes), jnp.float32),
        in_specs=[smem] + [vmem] * 4 + [hbm] * 8,
        out_specs=vmem,
        scratch_shapes=[
            pltpu.VMEM(x.shape, jnp.bfloat16),
            pltpu.VMEM((chunks, users, CHUNK, prefix), jnp.bfloat16),
            pltpu.VMEM((chunks, users, prefix, CHUNK), jnp.bfloat16),
            pltpu.VMEM((chunks, routers, matrices, share, CHUNK), jnp.bfloat16),
            pltpu.VMEM((cores, matrices, share, width), jnp.bfloat16),
            pltpu.VMEM(w_one.shape, jnp.bfloat16),
            pltpu.VMEM((room, width), jnp.bfloat16),
            pltpu.VMEM((TILE, width), jnp.bfloat16),
            pltpu.VMEM((TILE, width), jnp.float32),
            pltpu.VMEM((TILE, width), jnp.float32),
            pltpu.VMEM((room, lanes), jnp.int32),
            pltpu.VMEM((room, lanes), jnp.float32),
            pltpu.VMEM((rows, lanes), jnp.float32),
            pltpu.SMEM((units,), jnp.int32),
            pltpu.SMEM((units,), jnp.int32),
            pltpu.SemaphoreType.DMA((1,)),
            pltpu.SemaphoreType.DMA((chunks, routers + 2)),
            pltpu.SemaphoreType.DMA((cores, routers)),
            pltpu.SemaphoreType.DMA((1,)),
        ],
        compiler_params=pltpu.CompilerParams(vmem_limit_bytes=VMEM_LIMIT),
        name="score_units",
        interpret=INTERPRET,
    )(place_here, gain, gain2, mlp_gain, w_two, x, kt, kt2, values, values2, w, w2, w_one)


def local(
    items,
    block_owner,
    block_user,
    block_fill,
    prefix_keys,
    prefix_values,
    w_in,
    attn_gain,
    w_o,
    mlp_gain,
    w_one,
    w_two,
):
    blocks, block_width, model_width = items.shape
    peers = lax.axis_size("users")
    cores = lax.axis_size("heads")
    routers = lax.axis_size("routers")
    core = lax.axis_index("heads")
    flat_items = items.reshape(blocks * block_width, model_width)

    def swapped(x):
        return lax.ppermute(x, "heads", [(k, cores - 1 - k) for k in range(cores)])

    def exchanged(x):
        return lax.all_to_all(x, "users", split_axis=0, concat_axis=0, tiled=True)

    target = block_owner[:, 0]
    goes = target[None, :] == lax.broadcasted_iota(jnp.int32, (peers, blocks), 0)

    def rows_here(chosen):
        rows = jnp.sum(jnp.where(goes & chosen[None, :], block_fill[None, :], 0), axis=1)
        return (rows + (cores - 1 - core)) // cores

    index = jnp.arange(blocks, dtype=jnp.int32)
    same = target[:, None] == target[None, :]
    ahead = (block_user[None, :] < block_user[:, None]) | (
        (block_user[None, :] == block_user[:, None]) & (index[None, :] < index[:, None])
    )
    packed_start = jnp.sum(jnp.where(same & ahead, block_fill[None, :], 0), axis=1)
    inside = lax.broadcasted_iota(jnp.int32, (blocks, block_width), 1)
    packed = packed_start[:, None] + inside
    here = (inside < block_fill[:, None]) & (packed % cores == core)
    goes_to = jnp.where(here, target[:, None] * block_width + packed // cores, -1)
    goes_to = goes_to.reshape(1, blocks * block_width)
    slot = lax.broadcasted_iota(jnp.int32, (peers * block_width, 1), 0)
    sent = jnp.dot(
        (slot == goes_to).astype(jnp.bfloat16), flat_items, preferred_element_type=jnp.float32
    ).reshape(peers, block_width, model_width)
    sent = marked(sent, rows_here(block_user >= 0), rows_here(block_user == 0)).astype(jnp.bfloat16)
    sent, w_in = lax.optimization_barrier((sent, w_in))
    arrived = exchanged(sent)

    matrices, share, _ = w_in.shape
    w_local = jnp.concatenate([w_in, w_o.reshape(matrices, share, share)], axis=2)
    up = [(k, (k + 1) % routers) for k in range(routers)]
    down = [(k, (k - 1) % routers) for k in range(routers)]
    from_below, from_above = w_local, w_local
    ring = {0: w_local}
    for step in range(1, routers // 2):
        from_below = lax.ppermute(from_below, "routers", up)
        from_above = lax.ppermute(from_above, "routers", down)
        ring[routers - step] = from_below
        ring[step] = from_above
    half = matrices // 2
    lower = lax.ppermute(from_below[:half], "routers", up)
    upper = lax.ppermute(from_above[half:], "routers", down)
    ring[routers // 2] = jnp.concatenate([lower, upper], axis=0)
    w_ring = jnp.stack([ring[k] for k in range(routers)])
    own = (jnp.swapaxes(prefix_keys, 1, 2), prefix_values, attn_gain[None, :], w_ring)
    other = jax.tree.map(swapped, own)
    place_here = lax.axis_index("routers").astype(jnp.int32).reshape(1)
    scores = score_units(
        place_here, arrived, own, other, mlp_gain[None, :], w_one, w_two[None, :]
    ).reshape(peers, block_width)
    back = jnp.broadcast_to(scores[:, None, :], (peers, cores, block_width))
    returned = lax.all_to_all(
        back.reshape(peers * cores, block_width),
        ("users", "heads"),
        split_axis=0,
        concat_axis=0,
        tiled=True,
    ).reshape(peers, cores * block_width)
    row_scores = jnp.sum(jnp.where(goes[:, :, None], returned[:, None, :], 0.0), axis=0)
    lane = jnp.where(
        inside < block_fill[:, None], packed % cores * block_width + packed // cores, -1
    )
    wanted = lane[:, :, None] == lax.broadcasted_iota(
        jnp.int32, (blocks, block_width, cores * block_width), 2
    )
    return jnp.sum(jnp.where(wanted, row_scores[:, None, :], 0.0), axis=2)


def solution(mesh):
    placed = (
        P(("groups", "users", "routers"), None, None),
        P(("groups", "users", "routers"), None),
        P(("groups", "users", "routers")),
        P(("groups", "users", "routers")),
        P(("groups", "users"), None, "heads"),
        P(("groups", "users"), None, "heads"),
        P(None, "routers", "heads"),
        P("heads"),
        P("heads", "routers"),
        P(),
        P(),
        P(),
    )
    return jax.shard_map(
        local,
        mesh=mesh,
        in_specs=placed,
        out_specs=P(("groups", "users", "routers"), None),
        check_vma=False,
    )
```

```python
import jax
import jax.numpy as jnp
from jax import lax
from jax.experimental import pallas as pl
from jax.experimental.pallas import tpu as pltpu
from jax.sharding import PartitionSpec as P


HEAD_DIM = 128
EPSILON = 1e-05
TILE = 256
CHUNK = 256
ALIGN = 16
CODE = 128
UNUSED = 200.0
HEADER = 64.0
LOW = 32.0
HIGH = 4096.0
TINY = 2.0**-110
TINY_MARK = 2.0**14
LIFT = 2.0**125


def half_silu(half):
    return half * (1.0 + jnp.tanh(half))


def marked(rows, count, first):
    slots = rows.shape[1]
    slot = lax.broadcasted_iota(jnp.int32, rows.shape, 1)
    lane = lax.broadcasted_iota(jnp.int32, rows.shape, 2)
    count = count[:, None, None]
    first = first[:, None, None]
    last = slot == slots - 1
    unused = jnp.where(last, HEADER + first.astype(jnp.float32), UNUSED)
    lifted = jnp.where(jnp.abs(rows) < TINY, TINY_MARK, rows * LIFT)
    full = last & (count == slots)
    lift = full & (((lane == 0) & (first > 0)) | ((lane == 1) & (first == slots)))
    return jnp.where((slot >= count) & (lane == 0), unused, jnp.where(lift, lifted, rows))


def code_of(head):
    slots = head.shape[0]
    slot = lax.broadcasted_iota(jnp.int32, head.shape, 0)
    lane = lax.broadcasted_iota(jnp.int32, head.shape, 1)
    size = jnp.abs(head)
    valid = (size < LOW) | (size > HIGH)
    last = slot == slots - 1
    counts = jnp.where((lane == 0) & valid, 1.0, 0.0)
    header = jnp.where(last & (lane == 0) & ~valid, head - HEADER, 0.0)
    lifted = jnp.where(last & (lane <= 1) & (size > HIGH), slots / 2.0, 0.0)
    return jnp.sum(counts + CODE * (header + lifted))


def unmarked(rows):
    size = jnp.abs(rows)
    lowered = jnp.where(size < 2.0 * TINY_MARK, 0.0, rows * (1.0 / LIFT))
    return jnp.where(size > HIGH, lowered, rows)


def score_kernel(
    core_ref,
    gain_own,
    gain_other,
    mlp_gain_ref,
    w_two_ref,
    x_hbm,
    kt_own,
    kt_other,
    v_own,
    v_other,
    w_own,
    w_other,
    w_one_hbm,
    out_ref,
    x_ref,
    kt_ref,
    values_ref,
    w_ref,
    wo_ref,
    w_one_ref,
    rows_ref,
    prefix_ref,
    own_ref,
    gate_ref,
    user_ref,
    score_ref,
    unit_ref,
    offset_ref,
    code_ref,
    row_sem,
    chunk_sem,
    wo_sem,
    one_sem,
):
    units, unit_rows, width = x_hbm.shape
    routers, _, share, _ = w_own.shape
    half_width = v_own.shape[2]
    per_side = half_width // CHUNK
    chunks = width // CHUNK
    scale = HEAD_DIM ** (-0.5)
    router_here = core_ref[0]
    lanes = score_ref.shape[1]
    unit_row = lax.broadcasted_iota(jnp.int32, (unit_rows, lanes), 0)
    sides = ((kt_own, v_own, w_own), (kt_other, v_other, w_other))

    def ring_index(router):
        ahead = router - router_here
        return jnp.where(ahead < 0, ahead + routers, ahead)

    row_copy = pltpu.make_async_copy(x_hbm, x_ref, row_sem.at[0])
    row_copy.start()
    chunk_copies = []
    for chunk in range(chunks):
        kt, values, weights = sides[chunk // per_side]
        low = chunk % per_side * CHUNK
        copies = [
            pltpu.make_async_copy(
                weights.at[ring_index(router), :, :, low : low + CHUNK],
                w_ref.at[chunk, router],
                chunk_sem.at[chunk, router],
            )
            for router in range(routers)
        ]
        copies += [
            pltpu.make_async_copy(
                kt.at[:, low : low + CHUNK, :], kt_ref.at[chunk], chunk_sem.at[chunk, routers]
            ),
            pltpu.make_async_copy(
                values.at[:, :, low : low + CHUNK],
                values_ref.at[chunk],
                chunk_sem.at[chunk, routers + 1],
            ),
        ]
        for copy in copies:
            copy.start()
        chunk_copies.append(copies)
    tail_copies = []
    for side, (_, _, weights) in enumerate(sides):
        for router in range(routers):
            tail_copies.append(
                pltpu.make_async_copy(
                    weights.at[ring_index(router), :, :, half_width : half_width + share],
                    wo_ref.at[side, :, :, router * share : (router + 1) * share],
                    wo_sem.at[side, router],
                )
            )
    tail_copies.append(pltpu.make_async_copy(w_one_hbm, w_one_ref, one_sem.at[0]))
    for copy in tail_copies:
        copy.start()

    def place(unit, position):
        code = code_ref[unit]
        count = code % CODE
        first = code // CODE

        @pl.when(count > 0)
        def _():
            at = pl.multiple_of(position, ALIGN)
            rows_ref[pl.ds(at, unit_rows), :] = x_ref[unit]
            user_ref[pl.ds(at, unit_rows), :] = (unit_row >= first).astype(jnp.int32)

        offset_ref[unit] = position
        return position + (count + ALIGN - 1) // ALIGN * ALIGN

    row_copy.wait()
    for unit in range(units):
        head = x_ref[unit, :, 0:lanes].astype(jnp.float32)
        code_ref[unit] = code_of(head).astype(jnp.int32)
        x_ref[unit, :, 0:lanes] = unmarked(head).astype(jnp.bfloat16)
    total = lax.fori_loop(0, units, place, jnp.int32(0))

    def attend(user, queries, chunk, inner):
        raw = jnp.dot(
            queries,
            kt_ref[chunk, user, inner : inner + HEAD_DIM, :],
            preferred_element_type=jnp.float32,
        )
        weights = half_silu(raw * (0.5 * scale)).astype(jnp.bfloat16)
        return jnp.dot(
            weights,
            values_ref[chunk, user, :, inner : inner + HEAD_DIM],
            preferred_element_type=jnp.float32,
        )

    def tile_step(tile, wait):
        start = pl.multiple_of(tile * TILE, TILE)
        x = rows_ref[pl.ds(start, TILE), :]
        second = user_ref[pl.ds(start, TILE), :] > 0
        for chunk in range(chunks):
            at = chunk * CHUNK
            if wait:
                for copy in chunk_copies[chunk]:
                    copy.wait()

            def projected(which):
                weight = w_ref[chunk, :, which].reshape(width, CHUNK)
                return half_silu(jnp.dot(x, weight, preferred_element_type=jnp.float32) * 0.5)

            queries = projected(0).astype(jnp.bfloat16)
            keys = projected(1)
            values = projected(2)
            gate_ref[:, at : at + CHUNK] = projected(3)
            for inner in range(0, CHUNK, HEAD_DIM):
                part = slice(inner, inner + HEAD_DIM)
                place_at = slice(at + inner, at + inner + HEAD_DIM)
                raw = jnp.sum(
                    queries[:, part].astype(jnp.float32) * keys[:, part], axis=1, keepdims=True
                )
                own_ref[:, place_at] = half_silu(raw * (0.5 * scale)) * values[:, part]
                prefix_ref[:, place_at] = jnp.where(
                    second,
                    attend(1, queries[:, part], chunk, inner),
                    attend(0, queries[:, part], chunk, inner),
                ).astype(jnp.bfloat16)

        if wait:
            for copy in tail_copies:
                copy.wait()
        attended = prefix_ref[...].astype(jnp.float32) + own_ref[...]
        row_mean = jnp.sum(attended, axis=1, keepdims=True) / width
        row_var = jnp.sum(attended * attended, axis=1, keepdims=True) / width - row_mean * row_mean
        inverse = lax.rsqrt(row_var + EPSILON)
        residual = x.astype(jnp.float32)
        for side, gain_ref in enumerate((gain_own, gain_other)):
            part = slice(side * half_width, (side + 1) * half_width)
            gated = (
                (attended[:, part] - row_mean)
                * inverse
                * gain_ref[...].astype(jnp.float32)
                * gate_ref[:, part]
            ).astype(jnp.bfloat16)
            residual = residual + jnp.dot(
                gated,
                wo_ref[side].reshape(half_width, width),
                preferred_element_type=jnp.float32,
            )
        squares = jnp.sum(residual * residual, axis=1, keepdims=True)
        normed = (
            residual * lax.rsqrt(squares / width + EPSILON) * mlp_gain_ref[...].astype(jnp.float32)
        ).astype(jnp.bfloat16)
        inner_sum = jnp.dot(normed, w_one_ref[...], preferred_element_type=jnp.float32)
        hidden = half_silu(inner_sum * 0.5).astype(jnp.bfloat16).astype(jnp.float32)
        scores = jnp.sum(hidden * w_two_ref[...].astype(jnp.float32), axis=1, keepdims=True)
        score_ref[pl.ds(start, TILE), :] = jnp.broadcast_to(scores, (TILE, lanes))

    def later_tile(tile, carry):
        tile_step(tile, False)
        return carry

    tile_step(0, True)
    lax.fori_loop(1, (total + TILE - 1) // TILE, later_tile, 0)

    def unplace(unit, carry):
        count = code_ref[unit] % CODE
        to = pl.multiple_of(unit * unit_rows, unit_rows)

        @pl.when(count > 0)
        def _():
            at = pl.multiple_of(offset_ref[unit], ALIGN)
            found = score_ref[pl.ds(at, unit_rows), :]
            unit_ref[pl.ds(to, unit_rows), :] = jnp.where(unit_row < count, found, 0.0)

        @pl.when(count == 0)
        def _():
            unit_ref[pl.ds(to, unit_rows), :] = jnp.zeros((unit_rows, lanes), jnp.float32)

        return carry

    lax.fori_loop(0, units, unplace, 0)
    square = (lanes, lanes)
    diagonal = lax.broadcasted_iota(jnp.int32, square, 0) == lax.broadcasted_iota(
        jnp.int32, square, 1
    )
    for block in range(units * unit_rows // lanes):
        rows = unit_ref[block * lanes : (block + 1) * lanes, :]
        out_ref[block : block + 1, :] = jnp.sum(
            jnp.where(diagonal, rows, 0.0), axis=0, keepdims=True
        )


INTERPRET = False
VMEM_LIMIT = 40 * 1024 * 1024


def score_units(place_here, x, own, other, mlp_gain, w_one, w_two):
    units, unit_rows, width = x.shape
    kt, values, gain, w = own
    kt2, values2, gain2, w2 = other
    users, prefix, half_width = values.shape
    routers, matrices, share, _ = w.shape
    cores = width // half_width
    chunks = width // CHUNK
    lanes = 128
    rows = units * unit_rows
    room = (rows + TILE - 1) // TILE * TILE + max(TILE, unit_rows)
    smem = pl.BlockSpec(memory_space=pltpu.SMEM)
    vmem = pl.BlockSpec(memory_space=pltpu.VMEM)
    hbm = pl.BlockSpec(memory_space=pltpu.HBM)
    return pl.pallas_call(
        score_kernel,
        out_shape=jax.ShapeDtypeStruct((rows // lanes, lanes), jnp.float32),
        in_specs=[smem] + [vmem] * 4 + [hbm] * 8,
        out_specs=vmem,
        scratch_shapes=[
            pltpu.VMEM(x.shape, jnp.bfloat16),
            pltpu.VMEM((chunks, users, CHUNK, prefix), jnp.bfloat16),
            pltpu.VMEM((chunks, users, prefix, CHUNK), jnp.bfloat16),
            pltpu.VMEM((chunks, routers, matrices, share, CHUNK), jnp.bfloat16),
            pltpu.VMEM((cores, matrices, share, width), jnp.bfloat16),
            pltpu.VMEM(w_one.shape, jnp.bfloat16),
            pltpu.VMEM((room, width), jnp.bfloat16),
            pltpu.VMEM((TILE, width), jnp.bfloat16),
            pltpu.VMEM((TILE, width), jnp.float32),
            pltpu.VMEM((TILE, width), jnp.float32),
            pltpu.VMEM((room, lanes), jnp.int32),
            pltpu.VMEM((room, lanes), jnp.float32),
            pltpu.VMEM((rows, lanes), jnp.float32),
            pltpu.SMEM((units,), jnp.int32),
            pltpu.SMEM((units,), jnp.int32),
            pltpu.SemaphoreType.DMA((1,)),
            pltpu.SemaphoreType.DMA((chunks, routers + 2)),
            pltpu.SemaphoreType.DMA((cores, routers)),
            pltpu.SemaphoreType.DMA((1,)),
        ],
        compiler_params=pltpu.CompilerParams(vmem_limit_bytes=VMEM_LIMIT),
        name="score_units",
        interpret=INTERPRET,
    )(place_here, gain, gain2, mlp_gain, w_two, x, kt, kt2, values, values2, w, w2, w_one)


def local(
    items,
    block_owner,
    block_user,
    block_fill,
    prefix_keys,
    prefix_values,
    w_in,
    attn_gain,
    w_o,
    mlp_gain,
    w_one,
    w_two,
):
    blocks, block_width, model_width = items.shape
    peers = lax.axis_size("users")
    cores = lax.axis_size("heads")
    routers = lax.axis_size("routers")
    core = lax.axis_index("heads")
    flat_items = items.reshape(blocks * block_width, model_width)

    def swapped(x):
        return lax.ppermute(x, "heads", [(k, cores - 1 - k) for k in range(cores)])

    def exchanged(x):
        return lax.all_to_all(x, "users", split_axis=0, concat_axis=0, tiled=True)

    target = block_owner[:, 0]
    goes = target[None, :] == lax.broadcasted_iota(jnp.int32, (peers, blocks), 0)

    def rows_here(chosen):
        rows = jnp.sum(jnp.where(goes & chosen[None, :], block_fill[None, :], 0), axis=1)
        return (rows + (cores - 1 - core)) // cores

    index = jnp.arange(blocks, dtype=jnp.int32)
    same = target[:, None] == target[None, :]
    ahead = (block_user[None, :] < block_user[:, None]) | (
        (block_user[None, :] == block_user[:, None]) & (index[None, :] < index[:, None])
    )
    packed_start = jnp.sum(jnp.where(same & ahead, block_fill[None, :], 0), axis=1)
    inside = lax.broadcasted_iota(jnp.int32, (blocks, block_width), 1)
    packed = packed_start[:, None] + inside
    here = (inside < block_fill[:, None]) & (packed % cores == core)
    goes_to = jnp.where(here, target[:, None] * block_width + packed // cores, -1)
    goes_to = goes_to.reshape(1, blocks * block_width)
    slot = lax.broadcasted_iota(jnp.int32, (peers * block_width, 1), 0)
    sent = jnp.dot(
        (slot == goes_to).astype(jnp.bfloat16), flat_items, preferred_element_type=jnp.float32
    ).reshape(peers, block_width, model_width)
    sent = marked(sent, rows_here(block_user >= 0), rows_here(block_user == 0)).astype(jnp.bfloat16)
    sent, w_in = lax.optimization_barrier((sent, w_in))
    arrived = exchanged(sent)

    matrices, share, _ = w_in.shape
    w_local = jnp.concatenate([w_in, w_o.reshape(matrices, share, share)], axis=2)
    up = [(k, (k + 1) % routers) for k in range(routers)]
    down = [(k, (k - 1) % routers) for k in range(routers)]
    from_below, from_above = w_local, w_local
    ring = {0: w_local}
    for step in range(1, routers // 2):
        from_below = lax.ppermute(from_below, "routers", up)
        from_above = lax.ppermute(from_above, "routers", down)
        ring[routers - step] = from_below
        ring[step] = from_above
    half = matrices // 2
    lower = lax.ppermute(from_below[:half], "routers", up)
    upper = lax.ppermute(from_above[half:], "routers", down)
    ring[routers // 2] = jnp.concatenate([lower, upper], axis=0)
    w_ring = jnp.stack([ring[k] for k in range(routers)])
    own = (jnp.swapaxes(prefix_keys, 1, 2), prefix_values, attn_gain[None, :], w_ring)
    other = jax.tree.map(swapped, own)
    place_here = lax.axis_index("routers").astype(jnp.int32).reshape(1)
    scores = score_units(
        place_here, arrived, own, other, mlp_gain[None, :], w_one, w_two[None, :]
    ).reshape(peers, block_width)
    back = jnp.broadcast_to(scores[:, None, :], (peers, cores, block_width))
    returned = lax.all_to_all(
        back.reshape(peers * cores, block_width),
        ("users", "heads"),
        split_axis=0,
        concat_axis=0,
        tiled=True,
    ).reshape(peers, cores * block_width)
    row_scores = jnp.sum(jnp.where(goes[:, :, None], returned[:, None, :], 0.0), axis=0)
    lane = packed % cores * block_width + packed // cores
    wanted = lane[:, :, None] == lax.broadcasted_iota(
        jnp.int32, (blocks, block_width, cores * block_width), 2
    )
    block_scores = jnp.sum(jnp.where(wanted, row_scores[:, None, :], 0.0), axis=2)
    return jnp.where(inside < block_fill[:, None], block_scores, jnp.zeros_like(block_scores))


def solution(mesh):
    placed = (
        P(("groups", "users", "routers"), None, None),
        P(("groups", "users", "routers"), None),
        P(("groups", "users", "routers")),
        P(("groups", "users", "routers")),
        P(("groups", "users"), None, "heads"),
        P(("groups", "users"), None, "heads"),
        P(None, "routers", "heads"),
        P("heads"),
        P("heads", "routers"),
        P(),
        P(),
        P(),
    )
    return jax.shard_map(
        local,
        mesh=mesh,
        in_specs=placed,
        out_specs=P(("groups", "users", "routers"), None),
        check_vma=False,
    )
```
